512 devices in a mesh: dp: 4 (over y_lo, core), tp: 128 (over z, x, y_hi).
Axes of the slice: x: 4, y: 4 (y_hi: 2, y_lo: 2; y = y_hi * 2 + y_lo), z: 16, core: 2. Of those that a mesh axis runs over, the one named last changes fastest.
Arguments:
- inputs: bfloat16 [4, 128, 8192], P('dp', 'tp'), may hold values from -134 to 134, as said below
- norm_gain: float32 [8192], replicated, may hold values from 0.1 to 1.9
- gate_grad: bfloat16 [4, 128, 16384], P('dp', None, 'tp'), may hold values from -36 to 36
- up_grad: bfloat16 [4, 128, 16384], P('dp', None, 'tp'), may hold values from -36 to 36
- gate_weight: bfloat16 [8192, 16384], P(None, 'tp'), may hold values from -0.046875 to 0.046875
- up_weight: bfloat16 [8192, 16384], P(None, 'tp'), may hold values from -0.046875 to 0.046875
Outputs:
- input_grad: bfloat16 [4, 128, 8192], P('dp', 'tp')
- gain_grad: float32 [8192], replicated
The draws below stay inside these ranges and needn't reach their ends.
Inputs may be any that keep to these rules, and one draw needn't show every extreme that they name: `inputs`: activations with token and feature scales.
All inputs are finite; a program needn't handle non-finite values.
Results may differ from the reference program's by a relative error of at most 0.00165.
Values may be sent and summed in bfloat16 or wider, within the bound.
A program may use at most 64 MiB of HBM per device.

```python
import math
import jax
import jax.numpy as jnp
from jax import lax

D = 8192
FF = 16384
SEQ = 128
BATCH = 4


def draw_inputs(key, part):
    key_rows, key_cols, key_vals = jax.random.split(key, 3)
    row_scale = jnp.exp(jax.random.uniform(key_rows, (BATCH, SEQ, 1), jnp.float32, 0.0, math.log(10.0)))
    col_scale = jnp.exp(jax.random.uniform(key_cols, (1, 1, D), jnp.float32, 0.0, math.log(10.0)))
    sample = jnp.clip(jax.random.normal(key_vals, (BATCH, SEQ, D), jnp.float32), -4.0, 4.0)
    return (sample * row_scale * col_scale / 3.0).astype(jnp.bfloat16)


def cotangent(key, salt):
    key_cols, key_vals = jax.random.split(jax.random.fold_in(key, salt), 2)
    position = jnp.arange(SEQ, dtype=jnp.float32) / max(SEQ - 1, 1)
    col_scale = jnp.exp(jax.random.uniform(key_cols, (1, 1, FF), jnp.float32, math.log(0.3), math.log(3.0)))
    rising = 1.0 + 2.0 * position
    sample = jnp.clip(jax.random.normal(key_vals, (BATCH, SEQ, FF), jnp.float32), -4.0, 4.0)
    return (sample * rising[None, :, None] * col_scale).astype(jnp.bfloat16)


def draw_gate_grad(key, part):
    return cotangent(key, 11)


def draw_up_grad(key, part):
    return cotangent(key, 23)


def shard_levels(key, extent, cuts, smallest, top_value):
    factor_of = 1.0
    for dim, blocks in cuts:
        draws = jax.random.uniform(jax.random.fold_in(jax.random.fold_in(key, 6), dim), (blocks,), jnp.float32, smallest / len(cuts), top_value / len(cuts))
        factor_of = factor_of * jnp.repeat(jnp.exp(draws), extent[dim] // blocks).reshape((-1,) + (1,) * (len(extent) - 1 - dim))
    return factor_of


def bell_draw(key, extent, scale, most, cuts=(), held_as=jnp.bfloat16):
    values = jax.random.normal(key, extent, jnp.float32) * scale
    if len(cuts) > 0:
        values = shard_levels(key, extent, cuts, -0.22, 0.18) * values
    return jnp.clip(values, min=-most, max=most).astype(held_as)


def setup_inputs(seed: int = 0) -> dict:
    arg_keys = jax.random.split(jax.random.key(seed), 7)
    inputs = draw_inputs(jax.random.fold_in(arg_keys[6], 71), 0)
    norm_gain = jnp.clip(1.0 + 0.18 * jax.random.normal(arg_keys[1], (D,), jnp.float32), 0.1, 1.9)
    gate_grad = draw_gate_grad(jax.random.fold_in(arg_keys[6], 71), 0)
    up_grad = draw_up_grad(jax.random.fold_in(arg_keys[6], 71), 0)
    gate_weight = bell_draw(arg_keys[4], (D, FF), FF ** -0.5, 0.046875, ((1, 128),))
    up_weight = bell_draw(arg_keys[5], (D, FF), FF ** -0.5, 0.046875, ((1, 128),))
    return dict(inputs=inputs, norm_gain=norm_gain, gate_grad=gate_grad, up_grad=up_grad, gate_weight=gate_weight, up_weight=up_weight)


epsilon = 1e-05

def reference(inputs, norm_gain, gate_grad, up_grad, gate_weight, up_weight):
    values = inputs.astype(jnp.float32)
    inv_rms = lax.rsqrt(lax.optimization_barrier(jnp.mean(values * values, axis=-1, keepdims=True)) + epsilon)
    normed = values * inv_rms
    flat_gate = gate_grad.reshape(-1, gate_grad.shape[-1])
    flat_up = up_grad.reshape(-1, up_grad.shape[-1])
    dims = (((1,), (1,)), ((), ()))
    row_grad = lax.dot_general(flat_gate, gate_weight, dims, preferred_element_type=jnp.float32)
    row_grad = row_grad + lax.dot_general(flat_up, up_weight, dims, preferred_element_type=jnp.float32)
    row_grad = row_grad.reshape(inputs.shape)
    gain_grad = lax.optimization_barrier(jnp.sum(row_grad * normed, axis=(0, 1)))
    scaled = row_grad * norm_gain
    inner = lax.optimization_barrier(jnp.mean(scaled * normed, axis=-1, keepdims=True))
    input_grad = (inv_rms * (scaled - normed * inner)).astype(jnp.bfloat16)
    return (input_grad, gain_grad)
```

```python
import jax
import jax.numpy as jnp
from jax import lax
from jax.experimental import pallas as pl
from jax.experimental.pallas import tpu as pltpu
from jax.sharding import Mesh
from jax.sharding import PartitionSpec as P

TP = ("tp_0", "tp_1", "tp_2")
DP = ("dp_0", "dp_1")
MESH = pl.DeviceIdType.MESH

epsilon = 1e-05

D = 8192
NX = 4
NZ = 16
PARTS = 16
PW = D // PARTS
CH = 4
CW = PW // CH
X_ORDER = (1, 3, 2)
Z_DIRECT = (1, 2, 3, -1, -2, -3)
Z_RELAY = ((1, 5), (2, 6), (3, 7), (4, 8), (-1, -5), (-2, -6), (-3, -7))
NT = (((1,), (1,)), ((), ()))


def copy_to(src, dst, send, recv, device):
    copy = pltpu.make_async_remote_copy(
        src_ref=src, dst_ref=dst, send_sem=send, recv_sem=recv, device_id=device, device_id_type=MESH
    )
    copy.start()
    return copy


def wait_bytes(ref, sem):
    pltpu.make_async_copy(ref, ref, sem).wait()


def kernel(
    gw, uw, gg, ug, xin, gain, out, gout,
    cots, wst, wb, psend, pown, yr, qz, rdir, rrel, srel, r2, nown, nrecv, trow, rrow, gown, grecv, gsum, gall,
    w_sem, cx_send, cx_recv, cy_send, cy_recv, cc_send, cc_recv, wx_send, wx_recv, y_send, y_recv,
    zd_send, zd_recv, zr_send, zr_recv, z2_send, z2_recv, n_send, n_recv, t_send, t_recv, g_send, g_recv, a_send, a_recv,
):
    lo, co = lax.axis_index("dp_0"), lax.axis_index("dp_1")
    z, x, hi = lax.axis_index("tp_0"), lax.axis_index("tp_1"), lax.axis_index("tp_2")

    def dev(lo=lo, co=co, z=z, x=x, hi=hi):
        return {"dp_0": lo, "dp_1": co, "tp_0": z, "tp_1": x, "tp_2": hi}

    def at_x(r):
        return lax.rem(x + r, NX)

    def at_z(d):
        return lax.rem(z + (d + NZ), NZ)

    side = lax.rem(lo + hi, 2)

    def part(x, side, co):
        return (x * 2 + side) * 2 + co

    def group_peer(j):
        dx, dlo, dco = j // 4, (j // 2) % 2, j % 2
        px, plo, pco = lax.rem(x + dx, NX), lax.rem(lo + dlo, 2), lax.rem(co + dco, 2)
        return dev(lo=plo, co=pco, x=px), part(px, lax.rem(plo + hi, 2), pco), (plo * 2 + pco) * NX + px

    def far_peer(j):
        dz, dhi = j // 2, j % 2
        phi = lax.rem(hi + dhi, 2)
        return dev(lo=lax.rem(lo + dhi, 2), z=lax.rem(z + dz, NZ), hi=phi)

    mine = part(x, side, co)
    me = (lo * 2 + co) * NX + x
    seq = lo * 2 + co
    y_peer = dev(lo=1 - lo)
    core_peer = dev(co=1 - co)
    partner = dev(lo=1 - lo, hi=1 - hi)

    barrier = pltpu.get_barrier_semaphore()
    for j in range(1, 16):
        pl.semaphore_signal(barrier, inc=1, device_id=group_peer(j)[0], device_id_type=MESH)
    for j in range(1, 2 * NZ):
        pl.semaphore_signal(barrier, inc=1, device_id=far_peer(j), device_id_type=MESH)

    staged = []
    for r in X_ORDER + (0,):
        rows = pl.ds(pl.multiple_of(part(at_x(r), side, co) * PW, PW), PW)
        target = wb.at[0] if r == 0 else wst.at[r - 1]
        for i, w in enumerate((gw, uw)):
            copy = pltpu.make_async_copy(w.at[rows], target.at[:, pl.ds(128 * i, 128)], w_sem.at[r, i])
            copy.start()
            staged.append(copy)

    to = lax.broadcasted_iota(jnp.int32, (128, 128), 0)
    token = lax.broadcasted_iota(jnp.int32, (128, 128), 1)
    order = (token == 2 * (to % 64) + to // 64).astype(jnp.float32).astype(jnp.bfloat16)
    for i, c in enumerate((gg, ug)):
        ordered = jnp.dot(order, c[...], preferred_element_type=jnp.float32).astype(jnp.bfloat16)
        for h in range(2):
            cots[0, h, seq, :, 128 * i : 128 * (i + 1)] = ordered[64 * h : 64 * (h + 1)]

    total = jnp.zeros((1, PW), jnp.float32)
    for j in range(PARTS):
        v = xin[:, PW * j : PW * (j + 1)].astype(jnp.float32)
        total = total + v * v
    inv_rms = lax.rsqrt(jnp.sum(total, axis=-1, keepdims=True) / D + epsilon)
    for j in range(PARTS):
        nown[j] = xin[:, PW * j : PW * (j + 1)].astype(jnp.float32) * inv_rms

    pl.semaphore_wait(barrier, 15 + 2 * NZ - 1)

    sends = []
    own = cots.at[0, :, seq]
    for r in X_ORDER:
        sends.append(copy_to(own, cots.at[r, :, seq], cx_send.at[r - 1], cx_recv.at[r - 1], dev(x=at_x(r))))
    sends.append(copy_to(own, own, cy_send.at[0], cy_recv.at[0], y_peer))
    sends.append(copy_to(own, own, cc_send.at[0], cc_recv.at[0], core_peer))
    for i in range(8):
        staged[i].wait()
    for k in range(CH):
        rows = pl.ds(CW * k, CW)
        for r in X_ORDER:
            sends.append(
                copy_to(
                    wst.at[r - 1, rows], wb.at[r, rows], wx_send.at[r - 1, k], wx_recv.at[r - 1, k], dev(x=at_x(r))
                )
            )
    nrecv[me] = nown[mine]
    for j in range(1, 16):
        peer, theirs, _ = group_peer(j)
        copy_to(nown.at[theirs], nrecv.at[me], n_send, n_recv, peer)

    other = (1 - lo) * 2 + co
    for r in X_ORDER:
        block = cots.at[r, :, seq]
        sends[X_ORDER.index(r)].wait_recv()
        sends.append(copy_to(block, block, cy_send.at[r], cy_recv.at[r], y_peer))
        sends.append(copy_to(block, block, cc_send.at[r], cc_recv.at[r], core_peer))
    for r in (0,) + X_ORDER:
        block = cots.at[r, :, other]
        wait_bytes(block, cy_recv.at[r])
        sends.append(copy_to(block, block, cc_send.at[4 + r], cc_recv.at[4 + r], core_peer))
    for r in range(8):
        wait_bytes(cots.at[0, :, 0], cc_recv.at[r])

    def product(h, k):
        acc = jnp.zeros((256, CW), jnp.float32)
        for r in range(NX):
            rows = cots[r, h].reshape(256, 256)
            acc = acc + lax.dot_general(rows, wb[r, CW * k : CW * (k + 1)], NT, preferred_element_type=jnp.float32)
        return acc

    def multiply(k):
        for r in X_ORDER:
            wait_bytes(wb.at[r, pl.ds(CW * k, CW)], wx_recv.at[r - 1, k])
        psend[k] = product(1 - hi, k)
        sends.append(copy_to(psend.at[k], yr.at[k], y_send.at[k], y_recv.at[k], partner))
        pown[k] = product(hi, k)

    def add_y(k):
        wait_bytes(yr.at[k], y_recv.at[k])
        for b in range(NZ):
            for s in range(4):
                rows = slice(s * 64 + b * 4, s * 64 + b * 4 + 4)
                qz[k, b, 4 * s : 4 * s + 4] = pown[k, rows] + yr[k, rows]
        for i, (d, far) in enumerate(Z_RELAY):
            copy_to(qz.at[k, at_z(far)], rrel.at[k, i], zr_send.at[k], zr_recv.at[k], dev(z=at_z(d)))
        for i, d in enumerate(Z_DIRECT):
            copy_to(qz.at[k, at_z(d)], rdir.at[k, i], zd_send.at[k], zd_recv.at[k], dev(z=at_z(d)))

    def relay(k):
        wait_bytes(rrel.at[k], zr_recv.at[k])
        srel[k, 0] = qz[k, at_z(4)] + rrel[k, 0] + rrel[k, 1] + rrel[k, 2] + rrel[k, 3]
        srel[k, 1] = qz[k, at_z(-4)] + rrel[k, 4] + rrel[k, 5] + rrel[k, 6]
        copy_to(srel.at[k, 0], r2.at[k, 0], z2_send.at[k], z2_recv.at[k], dev(z=at_z(4)))
        copy_to(srel.at[k, 1], r2.at[k, 1], z2_send.at[k], z2_recv.at[k], dev(z=at_z(-4)))

    def add_z(k):
        wait_bytes(rdir.at[k], zd_recv.at[k])
        acc = qz[k, z]
        for i in range(6):
            acc = acc + rdir[k, i]
        wait_bytes(r2.at[k], z2_recv.at[k])
        acc = acc + r2[k, 0] + r2[k, 1]
        for i in range(16):
            trow[i, :, CW * k : CW * (k + 1)] = acc[i : i + 1]

    multiply(0)
    multiply(1)
    add_y(0)
    multiply(2)
    add_y(1)
    relay(0)
    multiply(3)
    add_y(2)
    relay(1)
    add_z(0)
    add_y(3)
    relay(2)
    add_z(1)
    relay(3)
    add_z(2)
    add_z(3)

    rrow[mine] = trow[me]
    for j in range(1, 16):
        peer, _, theirs = group_peer(j)
        copy_to(trow.at[theirs], rrow.at[mine], t_send, t_recv, peer)

    wait_bytes(nrecv.at[pl.ds(0, 15)], n_recv)
    acc = trow[0] * nrecv[0]
    for i in range(1, 16):
        acc = acc + trow[i] * nrecv[i]
    gown[...] = acc
    here = z * 2 + hi
    grecv[here] = acc
    for j in range(1, 2 * NZ):
        copy_to(gown, grecv.at[here], g_send, g_recv, far_peer(j))

    wait_bytes(rrow.at[pl.ds(0, 15)], t_recv)
    total = jnp.zeros((1, PW), jnp.float32)
    for j in range(PARTS):
        total = total + rrow[j] * gain[:, PW * j : PW * (j + 1)] * nown[j]
    inner = jnp.sum(total, axis=-1, keepdims=True) / D
    for j in range(PARTS):
        cols = slice(PW * j, PW * (j + 1))
        scaled = rrow[j] * gain[:, cols]
        out[:, cols] = (inv_rms * (scaled - nown[j] * inner)).astype(jnp.bfloat16)

    wait_bytes(grecv.at[pl.ds(0, 2 * NZ - 1)], g_recv)
    acc = grecv[0]
    for i in range(1, 2 * NZ):
        acc = acc + grecv[i]
    gsum[...] = acc
    gall[mine] = acc
    for j in range(1, 16):
        copy_to(gsum, gall.at[mine], a_send, a_recv, group_peer(j)[0])
    wait_bytes(gall.at[pl.ds(0, 15)], a_recv)
    for j in range(PARTS):
        gout[:, PW * j : PW * (j + 1)] = gall[j]

    for copy in sends:
        copy.wait_send()
    for k in range(CH):
        wait_bytes(rdir.at[k], zd_send.at[k])
        wait_bytes(rrel.at[k], zr_send.at[k])
        wait_bytes(r2.at[k], z2_send.at[k])
    wait_bytes(nrecv.at[pl.ds(0, 15)], n_send)
    wait_bytes(rrow.at[pl.ds(0, 15)], t_send)
    wait_bytes(grecv.at[pl.ds(0, 2 * NZ - 1)], g_send)
    wait_bytes(gall.at[pl.ds(0, 15)], a_send)


def per_device(inputs, norm_gain, gate_grad, up_grad, gate_weight, up_weight):
    f32, bf16 = jnp.float32, jnp.bfloat16
    dma = pltpu.SemaphoreType.DMA
    anywhere = pl.BlockSpec(memory_space=pl.ANY)
    vmem = pl.BlockSpec(memory_space=pltpu.VMEM)
    input_grad, gain_grad = pl.pallas_call(
        kernel,
        out_shape=(jax.ShapeDtypeStruct((1, D), bf16), jax.ShapeDtypeStruct((1, D), f32)),
        in_specs=[anywhere, anywhere, vmem, vmem, vmem, vmem],
        out_specs=(vmem, vmem),
        scratch_shapes=[
            pltpu.VMEM((NX, 2, 4, 64, 256), bf16),
            pltpu.VMEM((NX - 1, PW, 256), bf16),
            pltpu.VMEM((NX, PW, 256), bf16),
            pltpu.VMEM((CH, 256, CW), f32),
            pltpu.VMEM((CH, 256, CW), f32),
            pltpu.VMEM((CH, 256, CW), f32),
            pltpu.VMEM((CH, NZ, 16, CW), f32),
            pltpu.VMEM((CH, 6, 16, CW), f32),
            pltpu.VMEM((CH, 7, 16, CW), f32),
            pltpu.VMEM((CH, 2, 16, CW), f32),
            pltpu.VMEM((CH, 2, 16, CW), f32),
            pltpu.VMEM((PARTS, 1, PW), f32),
            pltpu.VMEM((16, 1, PW), f32),
            pltpu.VMEM((16, 1, PW), f32),
            pltpu.VMEM((PARTS, 1, PW), f32),
            pltpu.VMEM((1, PW), f32),
            pltpu.VMEM((2 * NZ, 1, PW), f32),
            pltpu.VMEM((1, PW), f32),
            pltpu.VMEM((PARTS, 1, PW), f32),
            dma((NX, 2)),
            dma((3,)), dma((3,)),
            dma((4,)), dma((4,)),
            dma((8,)), dma((8,)),
            dma((3, CH)), dma((3, CH)),
            dma((CH,)), dma((CH,)),
            dma((CH,)), dma((CH,)),
            dma((CH,)), dma((CH,)),
            dma((CH,)), dma((CH,)),
            dma, dma, dma, dma, dma, dma, dma, dma,
        ],
        compiler_params=pltpu.CompilerParams(collective_id=0, has_side_effects=True, vmem_limit_bytes=24 * 2**20),
    )(
        gate_weight,
        up_weight,
        gate_grad[0],
        up_grad[0],
        inputs[0],
        norm_gain.reshape(1, D),
    )
    return (input_grad[None], gain_grad.reshape(D))


def solution(mesh):
    finer = Mesh(mesh.devices.reshape(2, 2, NZ, NX, 2), ("dp_0", "dp_1", "tp_0", "tp_1", "tp_2"))
    return jax.shard_map(
        per_device,
        mesh=finer,
        in_specs=(P(DP, TP, None), P(), P(DP, None, TP), P(DP, None, TP), P(None, TP), P(None, TP)),
        out_specs=(P(DP, TP, None), P()),
        check_vma=False,
    )
```

```python
import jax
import jax.numpy as jnp
from jax import lax
from jax.experimental import pallas as pl
from jax.experimental.pallas import tpu as pltpu
from jax.sharding import Mesh
from jax.sharding import PartitionSpec as P

TP = ("tp_0", "tp_1", "tp_2")
DP = ("dp_0", "dp_1")
MESH = pl.DeviceIdType.MESH

epsilon = 1e-05

D = 8192
NX = 4
NZ = 16
PARTS = 16
PW = D // PARTS
CH = 4
CW = PW // CH
X_ORDER = (1, 3, 2)
Z_DIRECT = (1, 2, 3, -1, -2, -3)
Z_RELAY = ((1, 5), (2, 6), (3, 7), (4, 8), (-1, -5), (-2, -6), (-3, -7))
SCHEDULE = (
    ("forward_x", 1),
    ("forward_x", 3),
    ("forward_x", 2),
    ("forward_y", 0),
    ("forward_y", 1),
    ("forward_y", 3),
    ("near", 0),
    ("forward_y", 2),
    ("far", 0),
    ("near", 1),
    ("far", 1),
    ("add_y", 0),
    ("near", 2),
    ("far", 2),
    ("near", 3),
    ("far", 3),
    ("add_y", 1),
    ("relay", 0),
    ("add_y", 2),
    ("relay", 1),
    ("add_y", 3),
    ("add_z", 0),
    ("relay", 2),
    ("add_z", 1),
    ("relay", 3),
    ("add_z", 2),
    ("add_z", 3),
)
NT = (((1,), (1,)), ((), ()))


def copy_to(src, dst, send, recv, device):
    copy = pltpu.make_async_remote_copy(
        src_ref=src, dst_ref=dst, send_sem=send, recv_sem=recv, device_id=device, device_id_type=MESH
    )
    copy.start()
    return copy


def wait_bytes(ref, sem):
    pltpu.make_async_copy(ref, ref, sem).wait()


def kernel(
    gw, uw, gg_in, ug_in, x_in, gain_in, out, gout,
    gg, ug, xin, gain, cots, wst, wb, psend, pown, yr, qz, rdir, rrel, srel, r2, nown, nrecv, trow, rrow, gown, grecv, gsum, gall, gwait,
    k_sem, in_sem, w_sem, cx_send, cx_recv, cy_send, cy_recv, cc_send, cc_recv, wx_send, wx_recv, y_send, y_recv,
    zd_send, zd_recv, zr_send, zr_recv, z2_send, z2_recv, n_send, n_recv, t_send, t_recv, g_send, g_recv, a_send, a_recv,
):
    lo, co = lax.axis_index("dp_0"), lax.axis_index("dp_1")
    z, x, hi = lax.axis_index("tp_0"), lax.axis_index("tp_1"), lax.axis_index("tp_2")

    def dev(lo=lo, co=co, z=z, x=x, hi=hi):
        return {"dp_0": lo, "dp_1": co, "tp_0": z, "tp_1": x, "tp_2": hi}

    def at_x(r):
        return lax.rem(x + r, NX)

    def at_z(d):
        return lax.rem(z + (d + NZ), NZ)

    side = lax.rem(lo + hi, 2)

    def part(x, side, co):
        return (x * 2 + side) * 2 + co

    def group_peer(j):
        dx, dlo, dco = j // 4, (j // 2) % 2, j % 2
        px, plo, pco = lax.rem(x + dx, NX), lax.rem(lo + dlo, 2), lax.rem(co + dco, 2)
        return dev(lo=plo, co=pco, x=px), part(px, lax.rem(plo + hi, 2), pco), (plo * 2 + pco) * NX + px

    def plane_peer(j):
        dx, dlo, dco, dhi = j // 8, (j // 4) % 2, (j // 2) % 2, j % 2
        return dev(lo=lax.rem(lo + dlo, 2), co=lax.rem(co + dco, 2), x=lax.rem(x + dx, NX), hi=lax.rem(hi + dhi, 2))

    def greet(step, d):
        for away in (d, -d):
            pl.semaphore_signal(k_sem.at[step], inc=1, device_id=dev(z=at_z(away)), device_id_type=MESH)

    mine = part(x, side, co)
    me = (lo * 2 + co) * NX + x
    seq = lo * 2 + co
    y_peer = dev(lo=1 - lo)
    core_peer = dev(co=1 - co)
    partner = dev(lo=1 - lo, hi=1 - hi)

    with jax.named_scope("signals"):
        barrier = pltpu.get_barrier_semaphore()
        for j in range(1, 2 * 16):
            pl.semaphore_signal(barrier, inc=1, device_id=plane_peer(j), device_id_type=MESH)
        for away in (1, -1):
            pl.semaphore_signal(barrier, inc=1, device_id=dev(z=at_z(away)), device_id_type=MESH)

    loads = []
    for i, (src, dst) in enumerate(((gg_in, gg), (ug_in, ug), (x_in, xin), (gain_in, gain))):
        copy = pltpu.make_async_copy(src, dst, in_sem.at[i])
        copy.start()
        loads.append(copy)
    staged = []
    for r in X_ORDER + (0,):
        rows = pl.ds(pl.multiple_of(part(at_x(r), side, co) * PW, PW), PW)
        target = wb.at[0] if r == 0 else wst.at[r - 1]
        for i, w in enumerate((gw, uw)):
            copy = pltpu.make_async_copy(w.at[rows], target.at[:, pl.ds(128 * i, 128)], w_sem.at[r, i])
            copy.start()
            staged.append(copy)

    with jax.named_scope("prepare"):
        to = lax.broadcasted_iota(jnp.int32, (128, 128), 0)
        token = lax.broadcasted_iota(jnp.int32, (128, 128), 1)
        order = (token == 2 * (to % 64) + to // 64).astype(jnp.float32).astype(jnp.bfloat16)
        for i, c in enumerate((gg, ug)):
            loads[i].wait()
            ordered = jnp.dot(order, c[...], preferred_element_type=jnp.float32).astype(jnp.bfloat16)
            for h in range(2):
                cots[0, h, seq, :, 128 * i : 128 * (i + 1)] = ordered[64 * h : 64 * (h + 1)]

        loads[2].wait()
        loads[3].wait()
        total = jnp.zeros((1, PW), jnp.float32)
        for j in range(PARTS):
            v = xin[:, PW * j : PW * (j + 1)].astype(jnp.float32)
            total = total + v * v
        inv_rms = lax.rsqrt(jnp.sum(total, axis=-1, keepdims=True) / D + epsilon)
        for j in range(PARTS):
            nown[j] = xin[:, PW * j : PW * (j + 1)].astype(jnp.float32) * inv_rms

    with jax.named_scope("barrier"):
        pl.semaphore_wait(barrier, 31 + 2)
    greet(0, 1)

    sends = []
    with jax.named_scope("start_sends"):
        own = cots.at[0, :, seq]
        for r in X_ORDER:
            sends.append(copy_to(own, cots.at[r, :, seq], cx_send.at[r - 1], cx_recv.at[r - 1], dev(x=at_x(r))))
        sends.append(copy_to(own, own, cy_send.at[0], cy_recv.at[0], y_peer))
        sends.append(copy_to(own, own, cc_send.at[0], cc_recv.at[0], core_peer))
        for i in range(8):
            staged[i].wait()
        for k in range(CH):
            rows = pl.ds(CW * k, CW)
            for r in X_ORDER:
                sends.append(
                    copy_to(
                        wst.at[r - 1, rows], wb.at[r, rows], wx_send.at[r - 1, k], wx_recv.at[r - 1, k], dev(x=at_x(r))
                    )
                )
        nrecv[me] = nown[mine]
        for j in range(1, 16):
            peer, theirs, _ = group_peer(j)
            copy_to(nown.at[theirs], nrecv.at[me], n_send, n_recv, peer)

    other = (1 - lo) * 2 + co

    def forward_x(r):
        block = cots.at[r, :, seq]
        wait_bytes(block, cx_recv.at[r - 1])
        sends.append(copy_to(block, block, cy_send.at[r], cy_recv.at[r], y_peer))
        sends.append(copy_to(block, block, cc_send.at[r], cc_recv.at[r], core_peer))

    def forward_y(r):
        block = cots.at[r, :, other]
        wait_bytes(block, cy_recv.at[r])
        sends.append(copy_to(block, block, cc_send.at[4 + r], cc_recv.at[4 + r], core_peer))

    def product(h, l, k):
        acc = jnp.zeros((128, CW), jnp.float32)
        for r in range(NX):
            rows = cots[r, h, pl.ds(2 * l, 2)].reshape(128, 256)
            acc = acc + lax.dot_general(rows, wb[r, CW * k : CW * (k + 1)], NT, preferred_element_type=jnp.float32)
        return acc

    def multiply(l, b, k):
        if k == 0:
            for r in range(NX):
                wait_bytes(cots.at[0, :, 0], cc_recv.at[4 * b + r])
        if b == 0:
            for r in X_ORDER:
                wait_bytes(wb.at[r, pl.ds(CW * k, CW)], wx_recv.at[r - 1, k])
        psend[k, l] = product(1 - hi, l, k)
        sends.append(copy_to(psend.at[k, l], yr.at[k, l], y_send.at[k, b], y_recv.at[k, b], partner))
        pown[k, l] = product(hi, l, k)

    def multiply_near(k):
        multiply(lo, 0, k)

    def multiply_far(k):
        multiply(1 - lo, 1, k)

    def add_y(k):
        for b in range(2):
            wait_bytes(yr.at[k, 0], y_recv.at[k, b])
        for b in range(NZ):
            for s in range(4):
                rows = slice(s % 2 * 64 + b * 4, s % 2 * 64 + b * 4 + 4)
                qz[k, b, 4 * s : 4 * s + 4] = pown[k, s // 2, rows] + yr[k, s // 2, rows]
        if k == 0:
            pl.semaphore_wait(k_sem.at[1], 2)
            greet(2, 4)
        for i, (d, far) in enumerate(Z_RELAY):
            copy_to(qz.at[k, at_z(far)], rrel.at[k, i], zr_send.at[k], zr_recv.at[k], dev(z=at_z(d)))
        for i, d in enumerate(Z_DIRECT):
            copy_to(qz.at[k, at_z(d)], rdir.at[k, i], zd_send.at[k], zd_recv.at[k], dev(z=at_z(d)))

    def relay(k):
        wait_bytes(rrel.at[k], zr_recv.at[k])
        srel[k, 0] = qz[k, at_z(4)] + rrel[k, 0] + rrel[k, 1] + rrel[k, 2] + rrel[k, 3]
        srel[k, 1] = qz[k, at_z(-4)] + rrel[k, 4] + rrel[k, 5] + rrel[k, 6]
        copy_to(srel.at[k, 0], r2.at[k, 0], z2_send.at[k], z2_recv.at[k], dev(z=at_z(4)))
        copy_to(srel.at[k, 1], r2.at[k, 1], z2_send.at[k], z2_recv.at[k], dev(z=at_z(-4)))

    def add_z(k):
        wait_bytes(rdir.at[k], zd_recv.at[k])
        acc = qz[k, z]
        for i in range(6):
            acc = acc + rdir[k, i]
        wait_bytes(r2.at[k], z2_recv.at[k])
        acc = acc + r2[k, 0] + r2[k, 1]
        for i in range(16):
            trow[i, :, CW * k : CW * (k + 1)] = acc[i : i + 1]

    steps = {
        "forward_x": forward_x,
        "forward_y": forward_y,
        "near": multiply_near,
        "far": multiply_far,
        "add_y": add_y,
        "relay": relay,
        "add_z": add_z,
    }
    for step, k in SCHEDULE:
        with jax.named_scope(f"{step}_{k}"):
            if step == "near" and k == 0:
                pl.semaphore_wait(k_sem.at[0], 2)
                greet(1, 2)
            steps[step](k)

    with jax.named_scope("send_rows"):
        rrow[mine] = trow[me]
        for j in range(1, 16):
            peer, _, theirs = group_peer(j)
            copy_to(trow.at[theirs], rrow.at[mine], t_send, t_recv, peer)

    with jax.named_scope("gain_local"):
        wait_bytes(nrecv.at[pl.ds(0, 15)], n_recv)
        acc = trow[0] * nrecv[0]
        for i in range(1, 16):
            acc = acc + trow[i] * nrecv[i]
        gown[...] = acc
        grecv[z] = acc
        pl.semaphore_wait(k_sem.at[2], 2)
        for j in range(1, NZ):
            copy_to(gown, grecv.at[z], g_send, g_recv, dev(z=at_z(j)))

    with jax.named_scope("gain_far"):
        wait_bytes(grecv.at[pl.ds(0, NZ - 1)], g_recv)
        acc = grecv[0]
        for i in range(1, NZ):
            acc = acc + grecv[i]
        gsum[...] = acc
        gall[hi, mine] = acc
        for j in range(1, 2 * 16):
            copy_to(gsum, gall.at[hi, mine], a_send, a_recv, plane_peer(j))
    with jax.named_scope("rows"):
        wait_bytes(rrow.at[pl.ds(0, 15)], t_recv)
        total = jnp.zeros((1, PW), jnp.float32)
        for j in range(PARTS):
            total = total + rrow[j] * gain[:, PW * j : PW * (j + 1)] * nown[j]
        inner = jnp.sum(total, axis=-1, keepdims=True) / D
        for j in range(PARTS):
            cols = slice(PW * j, PW * (j + 1))
            scaled = rrow[j] * gain[:, cols]
            out[:, cols] = (inv_rms * (scaled - nown[j] * inner)).astype(jnp.bfloat16)

    with jax.named_scope("gain_all"):
        wait_bytes(gwait, a_recv)
        for j in range(PARTS):
            gout[:, PW * j : PW * (j + 1)] = gall[0, j] + gall[1, j]

    with jax.named_scope("drain"):
        for copy in sends:
            copy.wait_send()
        for k in range(CH):
            wait_bytes(rdir.at[k], zd_send.at[k])
            wait_bytes(rrel.at[k], zr_send.at[k])
            wait_bytes(r2.at[k], z2_send.at[k])
        wait_bytes(nrecv.at[pl.ds(0, 15)], n_send)
        wait_bytes(rrow.at[pl.ds(0, 15)], t_send)
        wait_bytes(grecv.at[pl.ds(0, NZ - 1)], g_send)
        wait_bytes(gwait, a_send)


def per_device(inputs, norm_gain, gate_grad, up_grad, gate_weight, up_weight):
    f32, bf16 = jnp.float32, jnp.bfloat16
    dma = pltpu.SemaphoreType.DMA
    hbm = pl.BlockSpec(memory_space=pl.ANY)
    vmem = pl.BlockSpec(memory_space=pltpu.VMEM)
    input_grad, gain_grad = pl.pallas_call(
        kernel,
        out_shape=(jax.ShapeDtypeStruct((1, D), bf16), jax.ShapeDtypeStruct((1, D), f32)),
        in_specs=[hbm] * 6,
        out_specs=(vmem, vmem),
        scratch_shapes=[
            pltpu.VMEM((128, 128), bf16),
            pltpu.VMEM((128, 128), bf16),
            pltpu.VMEM((1, D), bf16),
            pltpu.VMEM((1, D), f32),
            pltpu.VMEM((NX, 2, 4, 64, 256), bf16),
            pltpu.VMEM((NX - 1, PW, 256), bf16),
            pltpu.VMEM((NX, PW, 256), bf16),
            pltpu.VMEM((CH, 2, 128, CW), f32),
            pltpu.VMEM((CH, 2, 128, CW), f32),
            pltpu.VMEM((CH, 2, 128, CW), f32),
            pltpu.VMEM((CH, NZ, 16, CW), f32),
            pltpu.VMEM((CH, 6, 16, CW), f32),
            pltpu.VMEM((CH, 7, 16, CW), f32),
            pltpu.VMEM((CH, 2, 16, CW), f32),
            pltpu.VMEM((CH, 2, 16, CW), f32),
            pltpu.VMEM((PARTS, 1, PW), f32),
            pltpu.VMEM((16, 1, PW), f32),
            pltpu.VMEM((16, 1, PW), f32),
            pltpu.VMEM((PARTS, 1, PW), f32),
            pltpu.VMEM((1, PW), f32),
            pltpu.VMEM((NZ, 1, PW), f32),
            pltpu.VMEM((1, PW), f32),
            pltpu.VMEM((2, PARTS, 1, PW), f32),
            pltpu.VMEM((31, 1, PW), f32),
            pltpu.SemaphoreType.REGULAR((3,)),
            dma((4,)),
            dma((NX, 2)),
            dma((3,)), dma((3,)),
            dma((4,)), dma((4,)),
            dma((8,)), dma((8,)),
            dma((3, CH)), dma((3, CH)),
            dma((CH, 2)), dma((CH, 2)),
            dma((CH,)), dma((CH,)),
            dma((CH,)), dma((CH,)),
            dma((CH,)), dma((CH,)),
            dma, dma, dma, dma, dma, dma, dma, dma,
        ],
        compiler_params=pltpu.CompilerParams(collective_id=0, has_side_effects=True, vmem_limit_bytes=67_043_328),
    )(
        gate_weight,
        up_weight,
        gate_grad[0],
        up_grad[0],
        inputs[0],
        norm_gain.reshape(1, D),
    )
    return (input_grad[None], gain_grad.reshape(D))


def solution(mesh):
    finer = Mesh(mesh.devices.reshape(2, 2, NZ, NX, 2), ("dp_0", "dp_1", "tp_0", "tp_1", "tp_2"))
    return jax.shard_map(
        per_device,
        mesh=finer,
        in_specs=(P(DP, TP, None), P(), P(DP, None, TP), P(DP, None, TP), P(None, TP), P(None, TP)),
        out_specs=(P(DP, TP, None), P()),
        check_vma=False,
    )
```

```python
import jax
import jax.numpy as jnp
from jax import lax
from jax.experimental import pallas as pl
from jax.experimental.pallas import tpu as pltpu
from jax.sharding import Mesh
from jax.sharding import PartitionSpec as P

TP = ("tp_0", "tp_1", "tp_2")
DP = ("dp_0", "dp_1")
MESH = pl.DeviceIdType.MESH

epsilon = 1e-05

D = 8192
NX = 4
NZ = 16
PARTS = 16
PW = D // PARTS
CH = 4
CW = PW // CH
X_ORDER = (1, 3, 2)
Z_DIRECT = (1, 2, 3, -1, -2, -3)
Z_UP, Z_DOWN = ((1, 5), (2, 6), (3, 7)), ((-1, -5), (-2, -6), (-3, -7))
Z_RELAY = (Z_UP + ((4, 8),) + Z_DOWN, Z_DOWN + ((-4, -8),) + Z_UP)
XW = PW + 128
SCHEDULE = (
    ("forward_x", 1),
    ("forward_x", 3),
    ("forward_x", 2),
    ("forward_y", 0),
    ("gather", 0),
    ("forward_y", 1),
    ("forward_y", 3),
    ("near", 0),
    ("forward_y", 2),
    ("far", 0),
    ("near", 1),
    ("gather_on", 0),
    ("far", 1),
    ("add_y", 0),
    ("near", 2),
    ("far", 2),
    ("near", 3),
    ("far", 3),
    ("add_y", 1),
    ("relay", 0),
    ("normalize", 0),
    ("add_y", 2),
    ("relay", 1),
    ("add_y", 3),
    ("gain_local", 0),
    ("add_z", 0),
    ("relay", 2),
    ("add_z", 1),
    ("relay", 3),
    ("gain_far", 0),
    ("add_z", 2),
    ("add_z", 3),
)
NT = (((1,), (1,)), ((), ()))


def copy_to(src, dst, send, recv, device):
    copy = pltpu.make_async_remote_copy(
        src_ref=src, dst_ref=dst, send_sem=send, recv_sem=recv, device_id=device, device_id_type=MESH
    )
    copy.start()
    return copy


def wait_bytes(ref, sem):
    pltpu.make_async_copy(ref, ref, sem).wait()


def kernel(
    gw, uw, gg_in, ug_in, x_in, gain_in, out, gout,
    gg, ug, xin, gain, cots, wst, wb, psend, pown, yr, qz, rdir, rrel, srel, r2, nown, xsend, nrecv, xf, xz, nz, trow, rrow, gown, grecv, gsum, gall, gwait,
    k_sem, in_sem, w_sem, cx_send, cx_recv, cy_send, cy_recv, cc_send, cc_recv, wx_send, wx_recv, y_send, y_recv,
    zd_send, zd_recv, zr_send, zr_recv, z2_send, z2_recv, n_send, n_recv, v_send, v_recv, f_recv, t_send, t_recv, g_send, g_recv, a_send, a_recv,
):
    lo, co = lax.axis_index("dp_0"), lax.axis_index("dp_1")
    z, x, hi = lax.axis_index("tp_0"), lax.axis_index("tp_1"), lax.axis_index("tp_2")

    def dev(lo=lo, co=co, z=z, x=x, hi=hi):
        return {"dp_0": lo, "dp_1": co, "tp_0": z, "tp_1": x, "tp_2": hi}

    def at_x(r):
        return lax.rem(x + r, NX)

    def at_z(d):
        return lax.rem(z + (d + NZ), NZ)

    side = lax.rem(lo + hi, 2)

    def part(x, side, co):
        return (x * 2 + side) * 2 + co

    def group_peer(j):
        dx, dlo, dco = j // 4, (j // 2) % 2, j % 2
        px, plo, pco = lax.rem(x + dx, NX), lax.rem(lo + dlo, 2), lax.rem(co + dco, 2)
        return dev(lo=plo, co=pco, x=px), part(px, lax.rem(plo + hi, 2), pco), (plo * 2 + pco) * NX + px

    def plane_peer(j):
        dx, dlo, dco, dhi = j // 8, (j // 4) % 2, (j // 2) % 2, j % 2
        return dev(lo=lax.rem(lo + dlo, 2), co=lax.rem(co + dco, 2), x=lax.rem(x + dx, NX), hi=lax.rem(hi + dhi, 2))

    def greet(step, d):
        for away in (d, -d):
            pl.semaphore_signal(k_sem.at[step], inc=1, device_id=dev(z=at_z(away)), device_id_type=MESH)

    mine = part(x, side, co)
    me = (lo * 2 + co) * NX + x
    seq = lo * 2 + co
    y_peer = dev(lo=1 - lo)
    core_peer = dev(co=1 - co)
    partner = dev(lo=1 - lo, hi=1 - hi)

    with jax.named_scope("signals"):
        barrier = pltpu.get_barrier_semaphore()
        for j in range(1, 2 * 16):
            pl.semaphore_signal(barrier, inc=1, device_id=plane_peer(j), device_id_type=MESH)
        for away in (1, -1):
            pl.semaphore_signal(barrier, inc=1, device_id=dev(z=at_z(away)), device_id_type=MESH)

    loads = []
    for i, (src, dst) in enumerate(((gg_in, gg), (ug_in, ug), (x_in, xin), (gain_in, gain))):
        copy = pltpu.make_async_copy(src, dst, in_sem.at[i])
        copy.start()
        loads.append(copy)
    staged = []
    for r in X_ORDER + (0,):
        rows = pl.ds(pl.multiple_of(part(at_x(r), side, co) * PW, PW), PW)
        target = wb.at[0] if r == 0 else wst.at[r - 1]
        for i, w in enumerate((gw, uw)):
            copy = pltpu.make_async_copy(w.at[rows], target.at[:, pl.ds(128 * i, 128)], w_sem.at[r, i])
            copy.start()
            staged.append(copy)

    with jax.named_scope("prepare"):
        to = lax.broadcasted_iota(jnp.int32, (128, 128), 0)
        token = lax.broadcasted_iota(jnp.int32, (128, 128), 1)
        order = (token == 2 * (to % 64) + to // 64).astype(jnp.float32).astype(jnp.bfloat16)
        for i, c in enumerate((gg, ug)):
            loads[i].wait()
            ordered = jnp.dot(order, c[...], preferred_element_type=jnp.float32).astype(jnp.bfloat16)
            for h in range(2):
                cots[0, h, seq, :, 128 * i : 128 * (i + 1)] = ordered[64 * h : 64 * (h + 1)]

        loads[2].wait()
        loads[3].wait()
        total = jnp.zeros((1, PW), jnp.float32)
        for j in range(PARTS):
            v = xin[:, PW * j : PW * (j + 1)].astype(jnp.float32)
            total = total + v * v
        inv_rms = lax.rsqrt(jnp.sum(total, axis=-1, keepdims=True) / D + epsilon)
        for j in range(PARTS):
            v = xin[:, PW * j : PW * (j + 1)].astype(jnp.float32)
            nown[j] = v * inv_rms
            xsend[j, :, :PW] = v
            xsend[j, :, PW:] = jnp.broadcast_to(inv_rms, (1, 128))

    with jax.named_scope("barrier"):
        pl.semaphore_wait(barrier, 31 + 2)
    greet(0, 1)

    sends = []
    with jax.named_scope("start_sends"):
        own = cots.at[0, :, seq]
        for r in X_ORDER:
            sends.append(copy_to(own, cots.at[r, :, seq], cx_send.at[r - 1], cx_recv.at[r - 1], dev(x=at_x(r))))
        sends.append(copy_to(own, own, cy_send.at[0], cy_recv.at[0], y_peer))
        sends.append(copy_to(own, own, cc_send.at[0], cc_recv.at[0], core_peer))
        nrecv[me] = xsend[mine]
        for j in range(1, 16):
            peer, theirs, _ = group_peer(j)
            copy_to(xsend.at[theirs], nrecv.at[me], n_send, n_recv, peer)
        for i in range(8):
            staged[i].wait()
        for k in range(CH):
            rows = pl.ds(CW * k, CW)
            for r in X_ORDER:
                sends.append(
                    copy_to(
                        wst.at[r - 1, rows], wb.at[r, rows], wx_send.at[r - 1, k], wx_recv.at[r - 1, k], dev(x=at_x(r))
                    )
                )

    other = (1 - lo) * 2 + co

    def forward_x(r):
        block = cots.at[r, :, seq]
        wait_bytes(block, cx_recv.at[r - 1])
        sends.append(copy_to(block, block, cy_send.at[r], cy_recv.at[r], y_peer))
        sends.append(copy_to(block, block, cc_send.at[r], cc_recv.at[r], core_peer))

    def forward_y(r):
        block = cots.at[r, :, other]
        wait_bytes(block, cy_recv.at[r])
        sends.append(copy_to(block, block, cc_send.at[4 + r], cc_recv.at[4 + r], core_peer))

    def product(h, l, k):
        acc = jnp.zeros((128, CW), jnp.float32)
        for r in range(NX):
            rows = cots[r, h, pl.ds(2 * l, 2)].reshape(128, 256)
            acc = acc + lax.dot_general(rows, wb[r, CW * k : CW * (k + 1)], NT, preferred_element_type=jnp.float32)
        return acc

    def multiply(l, b, k):
        if k == 0:
            for r in range(NX):
                wait_bytes(cots.at[0, :, 0], cc_recv.at[4 * b + r])
        if b == 0:
            for r in X_ORDER:
                wait_bytes(wb.at[r, pl.ds(CW * k, CW)], wx_recv.at[r - 1, k])
        psend[k, l] = product(1 - hi, l, k)
        sends.append(copy_to(psend.at[k, l], yr.at[k, l], y_send.at[k, b], y_recv.at[k, b], partner))
        pown[k, l] = product(hi, l, k)

    def multiply_near(k):
        multiply(lo, 0, k)

    def multiply_far(k):
        multiply(1 - lo, 1, k)

    def add_y(k):
        for b in range(2):
            wait_bytes(yr.at[k, 0], y_recv.at[k, b])
        for b in range(NZ):
            for s in range(4):
                rows = slice(s % 2 * 64 + b * 4, s % 2 * 64 + b * 4 + 4)
                qz[k, b, 4 * s : 4 * s + 4] = pown[k, s // 2, rows] + yr[k, s // 2, rows]
        for i, (d, far) in enumerate(Z_RELAY[k % 2]):
            copy_to(qz.at[k, at_z(far)], rrel.at[k, i], zr_send.at[k], zr_recv.at[k], dev(z=at_z(d)))
        for i, d in enumerate(Z_DIRECT):
            copy_to(qz.at[k, at_z(d)], rdir.at[k, i], zd_send.at[k], zd_recv.at[k], dev(z=at_z(d)))

    def relay(k):
        wait_bytes(rrel.at[k], zr_recv.at[k])
        first = 4 if k % 2 == 0 else -4
        srel[k, 0] = qz[k, at_z(first)] + rrel[k, 0] + rrel[k, 1] + rrel[k, 2] + rrel[k, 3]
        srel[k, 1] = qz[k, at_z(-first)] + rrel[k, 4] + rrel[k, 5] + rrel[k, 6]
        copy_to(srel.at[k, 0], r2.at[k, 0], z2_send.at[k], z2_recv.at[k], dev(z=at_z(first)))
        copy_to(srel.at[k, 1], r2.at[k, 1], z2_send.at[k], z2_recv.at[k], dev(z=at_z(-first)))

    def add_z(k):
        wait_bytes(rdir.at[k], zd_recv.at[k])
        acc = qz[k, z]
        for i in range(6):
            acc = acc + rdir[k, i]
        wait_bytes(r2.at[k], z2_recv.at[k])
        acc = acc + r2[k, 0] + r2[k, 1]
        for i in range(16):
            trow[i, :, CW * k : CW * (k + 1)] = acc[i : i + 1]

    def gather(_):
        pl.semaphore_wait(k_sem.at[0], 2)
        greet(1, 2)
        wait_bytes(nrecv.at[pl.ds(0, 15)], n_recv)
        for i in range(16):
            xf[i : i + 1] = nrecv[i]
        xz[z, :, :PW] = xf[:, :PW].astype(jnp.bfloat16)
        inv = xf[:, PW:]
        high = inv.astype(jnp.bfloat16).astype(jnp.float32)
        middle = (inv - high).astype(jnp.bfloat16).astype(jnp.float32)
        low = inv - high - middle
        lane = lax.broadcasted_iota(jnp.int32, (16, 128), 1)
        split = jnp.where(lane == 0, high, jnp.where(lane == 1, middle, jnp.where(lane == 2, low, 0.0)))
        xz[z, :, PW:] = split.astype(jnp.bfloat16)
        pl.semaphore_wait(k_sem.at[1], 2)
        greet(2, 4)
        for i, d in enumerate((4, -4)):
            copy_to(xz.at[z], xz.at[z], v_send, f_recv.at[i], dev(z=at_z(d)))
        for d in Z_DIRECT:
            copy_to(xz.at[z], xz.at[z], v_send, v_recv, dev(z=at_z(d)))

    def gather_on(_):
        for i, (source, targets) in enumerate(((-4, (1, 2, 3, 4)), (4, (-1, -2, -3)))):
            block = xz.at[at_z(source)]
            wait_bytes(block, f_recv.at[i])
            for d in targets:
                copy_to(block, block, v_send, v_recv, dev(z=at_z(d)))

    def normalize(_):
        wait_bytes(xz.at[pl.ds(0, 13)], v_recv)
        for b in range(NZ):
            block = xz[b].astype(jnp.float32)
            nz[b] = block[:, :PW] * jnp.sum(block[:, PW:], axis=-1, keepdims=True)

    def gain_local(_):
        for k in range(CH):
            cols = slice(CW * k, CW * (k + 1))
            acc = qz[k, 0] * nz[0, :, cols]
            for b in range(1, NZ):
                acc = acc + qz[k, b] * nz[b, :, cols]
            gown[:, cols] = jnp.sum(acc, axis=0, keepdims=True)
        grecv[z] = gown[...]
        pl.semaphore_wait(k_sem.at[2], 2)
        for j in range(1, NZ):
            copy_to(gown, grecv.at[z], g_send, g_recv, dev(z=at_z(j)))

    def gain_far(_):
        wait_bytes(grecv.at[pl.ds(0, NZ - 1)], g_recv)
        acc = grecv[0]
        for i in range(1, NZ):
            acc = acc + grecv[i]
        gsum[...] = acc
        gall[hi, mine] = acc
        for j in range(1, 2 * 16):
            copy_to(gsum, gall.at[hi, mine], a_send, a_recv, plane_peer(j))

    steps = {
        "gather": gather,
        "gather_on": gather_on,
        "normalize": normalize,
        "gain_local": gain_local,
        "gain_far": gain_far,
        "forward_x": forward_x,
        "forward_y": forward_y,
        "near": multiply_near,
        "far": multiply_far,
        "add_y": add_y,
        "relay": relay,
        "add_z": add_z,
    }
    for step, k in SCHEDULE:
        with jax.named_scope(f"{step}_{k}"):
            steps[step](k)

    with jax.named_scope("send_rows"):
        rrow[mine] = trow[me]
        for j in range(1, 16):
            peer, _, theirs = group_peer(j)
            copy_to(trow.at[theirs], rrow.at[mine], t_send, t_recv, peer)

    with jax.named_scope("rows"):
        wait_bytes(rrow.at[pl.ds(0, 15)], t_recv)
        total = jnp.zeros((1, PW), jnp.float32)
        for j in range(PARTS):
            total = total + rrow[j] * gain[:, PW * j : PW * (j + 1)] * nown[j]
        inner = jnp.sum(total, axis=-1, keepdims=True) / D
        for j in range(PARTS):
            cols = slice(PW * j, PW * (j + 1))
            scaled = rrow[j] * gain[:, cols]
            out[:, cols] = (inv_rms * (scaled - nown[j] * inner)).astype(jnp.bfloat16)

    with jax.named_scope("gain_all"):
        wait_bytes(gwait, a_recv)
        for j in range(PARTS):
            gout[:, PW * j : PW * (j + 1)] = gall[0, j] + gall[1, j]

    with jax.named_scope("drain"):
        for copy in sends:
            copy.wait_send()
        for k in range(CH):
            wait_bytes(rdir.at[k], zd_send.at[k])
            wait_bytes(rrel.at[k], zr_send.at[k])
            wait_bytes(r2.at[k], z2_send.at[k])
        wait_bytes(nrecv.at[pl.ds(0, 15)], n_send)
        wait_bytes(xz.at[pl.ds(0, 15)], v_send)
        wait_bytes(rrow.at[pl.ds(0, 15)], t_send)
        wait_bytes(grecv.at[pl.ds(0, NZ - 1)], g_send)
        wait_bytes(gwait, a_send)


def per_device(inputs, norm_gain, gate_grad, up_grad, gate_weight, up_weight):
    f32, bf16 = jnp.float32, jnp.bfloat16
    dma = pltpu.SemaphoreType.DMA
    hbm = pl.BlockSpec(memory_space=pl.ANY)
    vmem = pl.BlockSpec(memory_space=pltpu.VMEM)
    input_grad, gain_grad = pl.pallas_call(
        kernel,
        out_shape=(jax.ShapeDtypeStruct((1, D), bf16), jax.ShapeDtypeStruct((1, D), f32)),
        in_specs=[hbm] * 6,
        out_specs=(vmem, vmem),
        scratch_shapes=[
            pltpu.VMEM((128, 128), bf16),
            pltpu.VMEM((128, 128), bf16),
            pltpu.VMEM((1, D), bf16),
            pltpu.VMEM((1, D), f32),
            pltpu.VMEM((NX, 2, 4, 64, 256), bf16),
            pltpu.VMEM((NX - 1, PW, 256), bf16),
            pltpu.VMEM((NX, PW, 256), bf16),
            pltpu.VMEM((CH, 2, 128, CW), f32),
            pltpu.VMEM((CH, 2, 128, CW), f32),
            pltpu.VMEM((CH, 2, 128, CW), f32),
            pltpu.VMEM((CH, NZ, 16, CW), f32),
            pltpu.VMEM((CH, 6, 16, CW), f32),
            pltpu.VMEM((CH, 7, 16, CW), f32),
            pltpu.VMEM((CH, 2, 16, CW), f32),
            pltpu.VMEM((CH, 2, 16, CW), f32),
            pltpu.VMEM((PARTS, 1, PW), f32),
            pltpu.VMEM((PARTS, 1, XW), f32),
            pltpu.VMEM((16, 1, XW), f32),
            pltpu.VMEM((16, XW), f32),
            pltpu.VMEM((NZ, 16, XW), bf16),
            pltpu.VMEM((NZ, 16, PW), f32),
            pltpu.VMEM((16, 1, PW), f32),
            pltpu.VMEM((PARTS, 1, PW), f32),
            pltpu.VMEM((1, PW), f32),
            pltpu.VMEM((NZ, 1, PW), f32),
            pltpu.VMEM((1, PW), f32),
            pltpu.VMEM((2, PARTS, 1, PW), f32),
            pltpu.VMEM((31, 1, PW), f32),
            pltpu.SemaphoreType.REGULAR((3,)),
            dma((4,)),
            dma((NX, 2)),
            dma((3,)), dma((3,)),
            dma((4,)), dma((4,)),
            dma((8,)), dma((8,)),
            dma((3, CH)), dma((3, CH)),
            dma((CH, 2)), dma((CH, 2)),
            dma((CH,)), dma((CH,)),
            dma((CH,)), dma((CH,)),
            dma((CH,)), dma((CH,)),
            dma, dma, dma, dma, dma((2,)),
            dma, dma, dma, dma, dma, dma,
        ],
        compiler_params=pltpu.CompilerParams(collective_id=0, has_side_effects=True, vmem_limit_bytes=67_043_328),
    )(
        gate_weight,
        up_weight,
        gate_grad[0],
        up_grad[0],
        inputs[0],
        norm_gain.reshape(1, D),
    )
    return (input_grad[None], gain_grad.reshape(D))


def solution(mesh):
    finer = Mesh(mesh.devices.reshape(2, 2, NZ, NX, 2), ("dp_0", "dp_1", "tp_0", "tp_1", "tp_2"))
    return jax.shard_map(
        per_device,
        mesh=finer,
        in_specs=(P(DP, TP, None), P(), P(DP, None, TP), P(DP, None, TP), P(None, TP), P(None, TP)),
        out_specs=(P(DP, TP, None), P()),
        check_vma=False,
    )
```

```python
import jax
import jax.numpy as jnp
from jax import lax
from jax.experimental import pallas as pl
from jax.experimental.pallas import tpu as pltpu
from jax.sharding import Mesh
from jax.sharding import PartitionSpec as P

TP = ("tp_0", "tp_1", "tp_2")
DP = ("dp_0", "dp_1")
MESH = pl.DeviceIdType.MESH

epsilon = 1e-05

D = 8192
NX = 4
NZ = 16
PARTS = 16
PW = D // PARTS
CH = 4
CW = PW // CH
X_ORDER = (1, 3, 2)
LEVELS = 240.0
MIDDLE = 120.0
Z_DIRECT = (1, 2, 3, -1, -2, -3)
Z_UP, Z_DOWN = ((1, 5), (2, 6), (3, 7)), ((-1, -5), (-2, -6), (-3, -7))
Z_RELAY = (Z_UP + ((4, 8),) + Z_DOWN, Z_DOWN + ((-4, -8),) + Z_UP)
XW = PW + 128
SCHEDULE = (
    ("forward_x", 1),
    ("forward_x", 3),
    ("forward_x", 2),
    ("forward_y", 0),
    ("gather", 0),
    ("forward_y", 1),
    ("near", 0),
    ("forward_y", 3),
    ("forward_y", 2),
    ("far", 0),
    ("near", 1),
    ("gather_on", 0),
    ("far", 1),
    ("add_y", 0),
    ("near", 2),
    ("far", 2),
    ("near", 3),
    ("far", 3),
    ("add_y", 1),
    ("relay", 0),
    ("normalize", 0),
    ("add_y", 2),
    ("relay", 1),
    ("add_y", 3),
    ("gain_local", 0),
    ("add_z", 0),
    ("relay", 2),
    ("add_z", 1),
    ("relay", 3),
    ("gain_far", 0),
    ("add_z", 2),
    ("add_z", 3),
)
NT = (((1,), (1,)), ((), ()))


def copy_to(src, dst, send, recv, device):
    copy = pltpu.make_async_remote_copy(
        src_ref=src, dst_ref=dst, send_sem=send, recv_sem=recv, device_id=device, device_id_type=MESH
    )
    copy.start()
    return copy


def encode(v):
    size = jnp.abs(v)
    top = jnp.maximum(jnp.max(size, axis=-1, keepdims=True) * 1.01, 1e-30)
    scale = top.astype(jnp.bfloat16).astype(jnp.float32)
    t = size * (LEVELS / scale)
    whole = jnp.floor(t)
    code = jnp.exp2(whole - MIDDLE) * (1.0 + (t - whole))
    return jnp.where(v < 0.0, -code, code).astype(jnp.bfloat16), scale


def decode(code, scale):
    code = code.astype(jnp.float32)
    size = jnp.abs(code)
    power = jnp.floor(jnp.log2(size))
    t = size * jnp.exp2(-power) + (power + (MIDDLE - 1.0))
    return jnp.where(code < 0.0, -t, t) * (scale * (1.0 / LEVELS))


def eye(rows):
    row = lax.broadcasted_iota(jnp.int32, (rows, 128), 0)
    lane = lax.broadcasted_iota(jnp.int32, (rows, 128), 1)
    return (row == lane).astype(jnp.float32)


def as_row(column):
    return jnp.sum(column * eye(column.shape[0]), axis=0, keepdims=True)


def as_column(row, rows):
    return jnp.sum(row * eye(rows), axis=-1, keepdims=True)


def wait_bytes(ref, sem):
    pltpu.make_async_copy(ref, ref, sem).wait()


def kernel(
    gw, uw, gg_in, ug_in, x_in, gain_in, out, gout,
    gg, ug, xin, gain, cots, wst, wb, psend, pown, yr, qz, qc, qs, rdir, rrel, srel, r2, srdir, srrel, ssrel, sr2, nown, xsend, nrecv, xf, xz, nz, trow, rrow, gown, grecv, gsum, gall, gwait,
    k_sem, in_sem, w_sem, cx_send, cx_recv, cy_send, cy_recv, cc_send, cc_recv, wx_send, wx_recv, y_send, y_recv,
    zd_send, zd_recv, zr_send, zr_recv, z2_send, z2_recv, szd_send, szd_recv, szr_send, szr_recv, sz2_send, sz2_recv, n_send, n_recv, v_send, v_recv, f_recv, t_send, t_recv, g_send, g_recv, a_send, a_recv,
):
    lo, co = lax.axis_index("dp_0"), lax.axis_index("dp_1")
    z, x, hi = lax.axis_index("tp_0"), lax.axis_index("tp_1"), lax.axis_index("tp_2")

    def dev(lo=lo, co=co, z=z, x=x, hi=hi):
        return {"dp_0": lo, "dp_1": co, "tp_0": z, "tp_1": x, "tp_2": hi}

    def at_x(r):
        return lax.rem(x + r, NX)

    def at_z(d):
        return lax.rem(z + (d + NZ), NZ)

    side = lax.rem(lo + hi, 2)

    def part(x, side, co):
        return (x * 2 + side) * 2 + co

    def group_peer(j):
        dx, dlo, dco = j // 4, (j // 2) % 2, j % 2
        px, plo, pco = lax.rem(x + dx, NX), lax.rem(lo + dlo, 2), lax.rem(co + dco, 2)
        return dev(lo=plo, co=pco, x=px), part(px, lax.rem(plo + hi, 2), pco), (plo * 2 + pco) * NX + px

    def plane_peer(j):
        dx, dlo, dco, dhi = j // 8, (j // 4) % 2, (j // 2) % 2, j % 2
        return dev(lo=lax.rem(lo + dlo, 2), co=lax.rem(co + dco, 2), x=lax.rem(x + dx, NX), hi=lax.rem(hi + dhi, 2))

    def greet(step, d):
        for away in (d, -d):
            pl.semaphore_signal(k_sem.at[step], inc=1, device_id=dev(z=at_z(away)), device_id_type=MESH)

    mine = part(x, side, co)
    me = (lo * 2 + co) * NX + x
    seq = lo * 2 + co
    y_peer = dev(lo=1 - lo)
    core_peer = dev(co=1 - co)
    partner = dev(lo=1 - lo, hi=1 - hi)

    with jax.named_scope("signals"):
        barrier = pltpu.get_barrier_semaphore()
        for j in range(1, 2 * 16):
            pl.semaphore_signal(barrier, inc=1, device_id=plane_peer(j), device_id_type=MESH)
        for away in (1, -1):
            pl.semaphore_signal(barrier, inc=1, device_id=dev(z=at_z(away)), device_id_type=MESH)

    loads = []
    for i, (src, dst) in enumerate(((gg_in, gg), (ug_in, ug), (x_in, xin), (gain_in, gain))):
        copy = pltpu.make_async_copy(src, dst, in_sem.at[i])
        copy.start()
        loads.append(copy)
    staged = []
    for r in X_ORDER + (0,):
        rows = pl.ds(pl.multiple_of(part(at_x(r), side, co) * PW, PW), PW)
        target = wb.at[0] if r == 0 else wst.at[r - 1]
        for i, w in enumerate((gw, uw)):
            copy = pltpu.make_async_copy(w.at[rows], target.at[:, pl.ds(128 * i, 128)], w_sem.at[r, i])
            copy.start()
            staged.append(copy)

    with jax.named_scope("prepare"):
        to = lax.broadcasted_iota(jnp.int32, (128, 128), 0)
        token = lax.broadcasted_iota(jnp.int32, (128, 128), 1)
        order = (token == 2 * (to % 64) + to // 64).astype(jnp.float32).astype(jnp.bfloat16)
        for i, c in enumerate((gg, ug)):
            loads[i].wait()
            ordered = jnp.dot(order, c[...], preferred_element_type=jnp.float32).astype(jnp.bfloat16)
            for h in range(2):
                cots[0, h, seq, :, 128 * i : 128 * (i + 1)] = ordered[64 * h : 64 * (h + 1)]

    with jax.named_scope("barrier"):
        pl.semaphore_wait(barrier, 31 + 2)
    greet(0, 1)

    sends = []
    with jax.named_scope("start_sends"):
        own = cots.at[0, :, seq]
        for r in X_ORDER:
            sends.append(copy_to(own, cots.at[r, :, seq], cx_send.at[r - 1], cx_recv.at[r - 1], dev(x=at_x(r))))
        sends.append(copy_to(own, own, cy_send.at[0], cy_recv.at[0], y_peer))
        sends.append(copy_to(own, own, cc_send.at[0], cc_recv.at[0], core_peer))
        loads[2].wait()
        loads[3].wait()
        total = jnp.zeros((1, PW), jnp.float32)
        for j in range(PARTS):
            v = xin[:, PW * j : PW * (j + 1)].astype(jnp.float32)
            total = total + v * v
        inv_rms = lax.rsqrt(jnp.sum(total, axis=-1, keepdims=True) / D + epsilon)
        for j in range(PARTS):
            v = xin[:, PW * j : PW * (j + 1)].astype(jnp.float32)
            nown[j] = v * inv_rms
            xsend[j, :, :PW] = v
            xsend[j, :, PW:] = jnp.broadcast_to(inv_rms, (1, 128))
        nrecv[me] = xsend[mine]
        for j in range(1, 16):
            peer, theirs, _ = group_peer(j)
            copy_to(xsend.at[theirs], nrecv.at[me], n_send, n_recv, peer)
        for i in range(8):
            staged[i].wait()
        for k in range(CH):
            rows = pl.ds(CW * k, CW)
            for r in X_ORDER:
                sends.append(
                    copy_to(
                        wst.at[r - 1, rows], wb.at[r, rows], wx_send.at[r - 1, k], wx_recv.at[r - 1, k], dev(x=at_x(r))
                    )
                )

    other = (1 - lo) * 2 + co

    def forward_x(r):
        block = cots.at[r, :, seq]
        wait_bytes(block, cx_recv.at[r - 1])
        sends.append(copy_to(block, block, cy_send.at[r], cy_recv.at[r], y_peer))
        sends.append(copy_to(block, block, cc_send.at[r], cc_recv.at[r], core_peer))

    def forward_y(r):
        block = cots.at[r, :, other]
        wait_bytes(block, cy_recv.at[r])
        sends.append(copy_to(block, block, cc_send.at[4 + r], cc_recv.at[4 + r], core_peer))

    def product(h, l, k):
        acc = jnp.zeros((128, CW), jnp.float32)
        for r in range(NX):
            rows = cots[r, h, pl.ds(2 * l, 2)].reshape(128, 256)
            acc = acc + lax.dot_general(rows, wb[r, CW * k : CW * (k + 1)], NT, preferred_element_type=jnp.float32)
        return acc

    def multiply(l, b, k):
        if k == 0:
            for r in range(NX):
                wait_bytes(cots.at[0, :, 0], cc_recv.at[4 * b + r])
        if b == 0:
            for r in X_ORDER:
                wait_bytes(wb.at[r, pl.ds(CW * k, CW)], wx_recv.at[r - 1, k])
        code, scale = encode(product(1 - hi, l, k))
        psend[k, l, :128] = code
        psend[k, l, 128:] = jnp.broadcast_to(as_row(scale), (16, 128)).astype(jnp.bfloat16)
        sends.append(copy_to(psend.at[k, l], yr.at[k, l], y_send.at[k, b], y_recv.at[k, b], partner))
        pown[k, l] = product(hi, l, k)

    def multiply_near(k):
        multiply(lo, 0, k)

    def multiply_far(k):
        multiply(1 - lo, 1, k)

    def add_y(k):
        for b in range(2):
            wait_bytes(yr.at[k, 0], y_recv.at[k, b])
        for l in range(2):
            scale = as_column(yr[k, l, 128:129].astype(jnp.float32), 128)
            pown[k, l] = pown[k, l] + decode(yr[k, l, :128], scale)
        for b in range(NZ):
            for s in range(4):
                rows = slice(s % 2 * 64 + b * 4, s % 2 * 64 + b * 4 + 4)
                qz[k, b, 4 * s : 4 * s + 4] = pown[k, s // 2, rows]
        code, scale = encode(qz[k])
        qc[k] = code
        qs[k] = jnp.sum(scale * eye(16), axis=1, keepdims=True)
        for i, (d, far) in enumerate(Z_RELAY[k % 2]):
            copy_to(qc.at[k, at_z(far)], rrel.at[k, i], zr_send.at[k], zr_recv.at[k], dev(z=at_z(d)))
            copy_to(qs.at[k, at_z(far)], srrel.at[k, i], szr_send.at[k], szr_recv.at[k], dev(z=at_z(d)))
        for i, d in enumerate(Z_DIRECT):
            copy_to(qc.at[k, at_z(d)], rdir.at[k, i], zd_send.at[k], zd_recv.at[k], dev(z=at_z(d)))
            copy_to(qs.at[k, at_z(d)], srdir.at[k, i], szd_send.at[k], szd_recv.at[k], dev(z=at_z(d)))

    def relay(k):
        wait_bytes(rrel.at[k], zr_recv.at[k])
        wait_bytes(srrel.at[k], szr_recv.at[k])
        first = 4 if k % 2 == 0 else -4
        for i, (d, sources) in enumerate(((first, (0, 1, 2, 3)), (-first, (4, 5, 6)))):
            acc = qz[k, at_z(d)]
            for j in sources:
                acc = acc + decode(rrel[k, j], as_column(srrel[k, j], 16))
            code, scale = encode(acc)
            srel[k, i] = code
            ssrel[k, i] = as_row(scale)
            copy_to(srel.at[k, i], r2.at[k, i], z2_send.at[k], z2_recv.at[k], dev(z=at_z(d)))
            copy_to(ssrel.at[k, i], sr2.at[k, i], sz2_send.at[k], sz2_recv.at[k], dev(z=at_z(d)))

    def add_z(k):
        wait_bytes(rdir.at[k], zd_recv.at[k])
        wait_bytes(srdir.at[k], szd_recv.at[k])
        acc = qz[k, z]
        for i in range(6):
            acc = acc + decode(rdir[k, i], as_column(srdir[k, i], 16))
        wait_bytes(r2.at[k], z2_recv.at[k])
        wait_bytes(sr2.at[k], sz2_recv.at[k])
        for i in range(2):
            acc = acc + decode(r2[k, i], as_column(sr2[k, i], 16))
        for i in range(16):
            trow[i, :, CW * k : CW * (k + 1)] = acc[i : i + 1]

    def gather(_):
        pl.semaphore_wait(k_sem.at[0], 2)
        greet(1, 2)
        wait_bytes(nrecv.at[pl.ds(0, 15)], n_recv)
        for i in range(16):
            xf[i : i + 1] = nrecv[i]
        xz[z, :, :PW] = xf[:, :PW].astype(jnp.bfloat16)
        inv = xf[:, PW:]
        high = inv.astype(jnp.bfloat16).astype(jnp.float32)
        middle = (inv - high).astype(jnp.bfloat16).astype(jnp.float32)
        low = inv - high - middle
        lane = lax.broadcasted_iota(jnp.int32, (16, 128), 1)
        split = jnp.where(lane == 0, high, jnp.where(lane == 1, middle, jnp.where(lane == 2, low, 0.0)))
        xz[z, :, PW:] = split.astype(jnp.bfloat16)
        pl.semaphore_wait(k_sem.at[1], 2)
        greet(2, 4)
        for i, d in enumerate((4, -4)):
            copy_to(xz.at[z], xz.at[z], v_send, f_recv.at[i], dev(z=at_z(d)))
        for d in Z_DIRECT:
            copy_to(xz.at[z], xz.at[z], v_send, v_recv, dev(z=at_z(d)))

    def gather_on(_):
        for i, (source, targets) in enumerate(((-4, (1, 2, 3, 4)), (4, (-1, -2, -3)))):
            block = xz.at[at_z(source)]
            wait_bytes(block, f_recv.at[i])
            for d in targets:
                copy_to(block, block, v_send, v_recv, dev(z=at_z(d)))

    def normalize(_):
        wait_bytes(xz.at[pl.ds(0, 13)], v_recv)
        for b in range(NZ):
            block = xz[b].astype(jnp.float32)
            nz[b] = block[:, :PW] * jnp.sum(block[:, PW:], axis=-1, keepdims=True)

    def gain_local(_):
        for k in range(CH):
            cols = slice(CW * k, CW * (k + 1))
            acc = qz[k, 0] * nz[0, :, cols]
            for b in range(1, NZ):
                acc = acc + qz[k, b] * nz[b, :, cols]
            gown[:, cols] = jnp.sum(acc, axis=0, keepdims=True)
        grecv[z] = gown[...]
        pl.semaphore_wait(k_sem.at[2], 2)
        for j in range(1, NZ):
            copy_to(gown, grecv.at[z], g_send, g_recv, dev(z=at_z(j)))

    def gain_far(_):
        wait_bytes(grecv.at[pl.ds(0, NZ - 1)], g_recv)
        acc = grecv[0]
        for i in range(1, NZ):
            acc = acc + grecv[i]
        gsum[...] = acc
        gall[hi, mine] = acc
        for j in range(1, 2 * 16):
            copy_to(gsum, gall.at[hi, mine], a_send, a_recv, plane_peer(j))

    steps = {
        "gather": gather,
        "gather_on": gather_on,
        "normalize": normalize,
        "gain_local": gain_local,
        "gain_far": gain_far,
        "forward_x": forward_x,
        "forward_y": forward_y,
        "near": multiply_near,
        "far": multiply_far,
        "add_y": add_y,
        "relay": relay,
        "add_z": add_z,
    }
    for step, k in SCHEDULE:
        with jax.named_scope(f"{step}_{k}"):
            steps[step](k)

    with jax.named_scope("send_rows"):
        rrow[mine] = trow[me]
        for j in range(1, 16):
            peer, _, theirs = group_peer(j)
            copy_to(trow.at[theirs], rrow.at[mine], t_send, t_recv, peer)

    with jax.named_scope("rows"):
        wait_bytes(rrow.at[pl.ds(0, 15)], t_recv)
        total = jnp.zeros((1, PW), jnp.float32)
        for j in range(PARTS):
            total = total + rrow[j] * gain[:, PW * j : PW * (j + 1)] * nown[j]
        inner = jnp.sum(total, axis=-1, keepdims=True) / D
        for j in range(PARTS):
            cols = slice(PW * j, PW * (j + 1))
            scaled = rrow[j] * gain[:, cols]
            out[:, cols] = (inv_rms * (scaled - nown[j] * inner)).astype(jnp.bfloat16)

    with jax.named_scope("gain_all"):
        wait_bytes(gwait, a_recv)
        for j in range(PARTS):
            gout[:, PW * j : PW * (j + 1)] = gall[0, j] + gall[1, j]

    with jax.named_scope("drain"):
        for copy in sends:
            copy.wait_send()
        for k in range(CH):
            wait_bytes(rdir.at[k], zd_send.at[k])
            wait_bytes(rrel.at[k], zr_send.at[k])
            wait_bytes(r2.at[k], z2_send.at[k])
            wait_bytes(srdir.at[k], szd_send.at[k])
            wait_bytes(srrel.at[k], szr_send.at[k])
            wait_bytes(sr2.at[k], sz2_send.at[k])
        wait_bytes(nrecv.at[pl.ds(0, 15)], n_send)
        wait_bytes(xz.at[pl.ds(0, 15)], v_send)
        wait_bytes(rrow.at[pl.ds(0, 15)], t_send)
        wait_bytes(grecv.at[pl.ds(0, NZ - 1)], g_send)
        wait_bytes(gwait, a_send)


def per_device(inputs, norm_gain, gate_grad, up_grad, gate_weight, up_weight):
    f32, bf16 = jnp.float32, jnp.bfloat16
    dma = pltpu.SemaphoreType.DMA
    hbm = pl.BlockSpec(memory_space=pl.ANY)
    vmem = pl.BlockSpec(memory_space=pltpu.VMEM)
    input_grad, gain_grad = pl.pallas_call(
        kernel,
        out_shape=(jax.ShapeDtypeStruct((1, D), bf16), jax.ShapeDtypeStruct((1, D), f32)),
        in_specs=[hbm] * 6,
        out_specs=(vmem, vmem),
        scratch_shapes=[
            pltpu.VMEM((128, 128), bf16),
            pltpu.VMEM((128, 128), bf16),
            pltpu.VMEM((1, D), bf16),
            pltpu.VMEM((1, D), f32),
            pltpu.VMEM((NX, 2, 4, 64, 256), bf16),
            pltpu.VMEM((NX - 1, PW, 256), bf16),
            pltpu.VMEM((NX, PW, 256), bf16),
            pltpu.VMEM((CH, 2, 144, CW), bf16),
            pltpu.VMEM((CH, 2, 128, CW), f32),
            pltpu.VMEM((CH, 2, 144, CW), bf16),
            pltpu.VMEM((CH, NZ, 16, CW), f32),
            pltpu.VMEM((CH, NZ, 16, CW), bf16),
            pltpu.VMEM((CH, NZ, 1, 128), f32),
            pltpu.VMEM((CH, 6, 16, CW), bf16),
            pltpu.VMEM((CH, 7, 16, CW), bf16),
            pltpu.VMEM((CH, 2, 16, CW), bf16),
            pltpu.VMEM((CH, 2, 16, CW), bf16),
            pltpu.VMEM((CH, 6, 1, 128), f32),
            pltpu.VMEM((CH, 7, 1, 128), f32),
            pltpu.VMEM((CH, 2, 1, 128), f32),
            pltpu.VMEM((CH, 2, 1, 128), f32),
            pltpu.VMEM((PARTS, 1, PW), f32),
            pltpu.VMEM((PARTS, 1, XW), f32),
            pltpu.VMEM((16, 1, XW), f32),
            pltpu.VMEM((16, XW), f32),
            pltpu.VMEM((NZ, 16, XW), bf16),
            pltpu.VMEM((NZ, 16, PW), f32),
            pltpu.VMEM((16, 1, PW), f32),
            pltpu.VMEM((PARTS, 1, PW), f32),
            pltpu.VMEM((1, PW), f32),
            pltpu.VMEM((NZ, 1, PW), f32),
            pltpu.VMEM((1, PW), f32),
            pltpu.VMEM((2, PARTS, 1, PW), f32),
            pltpu.VMEM((31, 1, PW), f32),
            pltpu.SemaphoreType.REGULAR((3,)),
            dma((4,)),
            dma((NX, 2)),
            dma((3,)), dma((3,)),
            dma((4,)), dma((4,)),
            dma((8,)), dma((8,)),
            dma((3, CH)), dma((3, CH)),
            dma((CH, 2)), dma((CH, 2)),
            dma((CH,)), dma((CH,)),
            dma((CH,)), dma((CH,)),
            dma((CH,)), dma((CH,)),
            dma((CH,)), dma((CH,)),
            dma((CH,)), dma((CH,)),
            dma((CH,)), dma((CH,)),
            dma, dma, dma, dma, dma((2,)),
            dma, dma, dma, dma, dma, dma,
        ],
        compiler_params=pltpu.CompilerParams(collective_id=0, has_side_effects=True, vmem_limit_bytes=67_043_328),
    )(
        gate_weight,
        up_weight,
        gate_grad[0],
        up_grad[0],
        inputs[0],
        norm_gain.reshape(1, D),
    )
    return (input_grad[None], gain_grad.reshape(D))


def solution(mesh):
    finer = Mesh(mesh.devices.reshape(2, 2, NZ, NX, 2), ("dp_0", "dp_1", "tp_0", "tp_1", "tp_2"))
    return jax.shard_map(
        per_device,
        mesh=finer,
        in_specs=(P(DP, TP, None), P(), P(DP, None, TP), P(DP, None, TP), P(None, TP), P(None, TP)),
        out_specs=(P(DP, TP, None), P()),
        check_vma=False,
    )
```

```python
import jax
import jax.numpy as jnp
from jax import lax
from jax.experimental import pallas as pl
from jax.experimental.pallas import tpu as pltpu
from jax.sharding import Mesh
from jax.sharding import PartitionSpec as P

TP = ("tp_0", "tp_1", "tp_2")
DP = ("dp_0", "dp_1")
MESH = pl.DeviceIdType.MESH

epsilon = 1e-05

D = 8192
NX = 4
NZ = 16
PARTS = 16
PW = D // PARTS
CH = 4
CW = PW // CH
X_ORDER = (1, 3, 2)
VMEM_GRANT = 55150 * 1024
LEVELS = 240.0
MIDDLE = 120.0
Z_DIRECT = (1, 2, 3, -1, -2, -3)
Z_UP, Z_DOWN = ((1, 5), (2, 6), (3, 7)), ((-1, -5), (-2, -6), (-3, -7))
Z_RELAY = (Z_UP + ((4, 8),) + Z_DOWN, Z_DOWN + ((-4, -8),) + Z_UP)
XW = PW + 128
SCHEDULE = (
    ("gather", 0),
    ("forward_x", 1),
    ("forward_x", 3),
    ("forward_x", 2),
    ("forward_y", 0),
    ("forward_y", 1),
    ("near", 0),
    ("forward_y", 3),
    ("forward_y", 2),
    ("far", 0),
    ("own", 0),
    ("gather_on", 0),
    ("near", 1),
    ("far", 1),
    ("own", 1),
    ("add_y", 0),
    ("near", 2),
    ("far", 2),
    ("own", 2),
    ("near", 3),
    ("far", 3),
    ("own", 3),
    ("add_y", 1),
    ("add_y", 2),
    ("relay", 0),
    ("add_y", 3),
    ("normalize", 0),
    ("gain_local", 0),
    ("relay", 1),
    ("relay", 2),
    ("relay", 3),
    ("add_z", 0),
    ("add_z", 1),
    ("add_z", 2),
    ("gain_far", 0),
    ("add_z", 3),
)
NT = (((1,), (1,)), ((), ()))


def copy_to(src, dst, send, recv, device):
    copy = pltpu.make_async_remote_copy(
        src_ref=src, dst_ref=dst, send_sem=send, recv_sem=recv, device_id=device, device_id_type=MESH
    )
    copy.start()
    return copy


def encode(v):
    size = jnp.abs(v)
    top = jnp.maximum(jnp.max(size, axis=-1, keepdims=True) * 1.01, 1e-30)
    scale = top.astype(jnp.bfloat16).astype(jnp.float32)
    t = size * (LEVELS / scale)
    whole = jnp.floor(t)
    code = jnp.exp2(whole - MIDDLE) * (1.0 + (t - whole))
    return jnp.where(v < 0.0, -code, code).astype(jnp.bfloat16), scale


def decode(code, scale):
    code = code.astype(jnp.float32)
    size = jnp.abs(code)
    power = jnp.floor(jnp.log2(size))
    t = size * jnp.exp2(-power) + (power + (MIDDLE - 1.0))
    return jnp.where(code < 0.0, -t, t) * (scale * (1.0 / LEVELS))


def eye(rows):
    row = lax.broadcasted_iota(jnp.int32, (rows, 128), 0)
    lane = lax.broadcasted_iota(jnp.int32, (rows, 128), 1)
    return (row == lane).astype(jnp.float32)


def as_row(column):
    return jnp.sum(column * eye(column.shape[0]), axis=0, keepdims=True)


def as_column(row, rows):
    return jnp.sum(row * eye(rows), axis=-1, keepdims=True)


def wait_bytes(ref, sem):
    pltpu.make_async_copy(ref, ref, sem).wait()


def kernel(
    gw, uw, gg_in, ug_in, x_in, gain_in, out, gout,
    gg, ug, xin, gain, cots, wst, wb, psend, pown, yr, qz, qc, qs, rdir, rrel, srel, r2, srdir, srrel, ssrel, sr2, nown, xsend, nrecv, xf, xz, nz, trow, rrow, gown, grecv, gsum, gall, gwait,
    k_sem, in_sem, w_sem, cx_send, cx_recv, cy_send, cy_recv, cc_send, cc_recv, wx_send, wx_recv, y_send, y_recv,
    zd_send, zd_recv, zr_send, zr_recv, z2_send, z2_recv, szd_send, szd_recv, szr_send, szr_recv, sz2_send, sz2_recv, n_send, n_recv, v_send, v_recv, f_recv, t_send, t_recv, g_send, g_recv, a_send, a_recv,
):
    lo, co = lax.axis_index("dp_0"), lax.axis_index("dp_1")
    z, x, hi = lax.axis_index("tp_0"), lax.axis_index("tp_1"), lax.axis_index("tp_2")

    def dev(lo=lo, co=co, z=z, x=x, hi=hi):
        return {"dp_0": lo, "dp_1": co, "tp_0": z, "tp_1": x, "tp_2": hi}

    def at_x(r):
        return lax.rem(x + r, NX)

    def at_z(d):
        return lax.rem(z + (d + NZ), NZ)

    side = lax.rem(lo + hi, 2)

    def part(x, side, co):
        return (x * 2 + side) * 2 + co

    def group_peer(j):
        dx, dlo, dco = j // 4, (j // 2) % 2, j % 2
        px, plo, pco = lax.rem(x + dx, NX), lax.rem(lo + dlo, 2), lax.rem(co + dco, 2)
        return dev(lo=plo, co=pco, x=px), part(px, lax.rem(plo + hi, 2), pco), (plo * 2 + pco) * NX + px

    def plane_peer(j):
        dx, dlo, dco, dhi = j // 8, (j // 4) % 2, (j // 2) % 2, j % 2
        return dev(lo=lax.rem(lo + dlo, 2), co=lax.rem(co + dco, 2), x=lax.rem(x + dx, NX), hi=lax.rem(hi + dhi, 2))

    def greet(step, d):
        for away in (d, -d):
            pl.semaphore_signal(k_sem.at[step], inc=1, device_id=dev(z=at_z(away)), device_id_type=MESH)

    mine = part(x, side, co)
    me = (lo * 2 + co) * NX + x
    seq = lo * 2 + co
    y_peer = dev(lo=1 - lo)
    core_peer = dev(co=1 - co)
    partner = dev(lo=1 - lo, hi=1 - hi)

    loads = []
    for i, (src, dst) in enumerate(((gg_in, gg), (ug_in, ug), (x_in, xin), (gain_in, gain))):
        copy = pltpu.make_async_copy(src, dst, in_sem.at[i])
        copy.start()
        loads.append(copy)
    with jax.named_scope("signals"):
        barrier = pltpu.get_barrier_semaphore()
        for j in range(1, 2 * 16):
            pl.semaphore_signal(barrier, inc=1, device_id=plane_peer(j), device_id_type=MESH)
        for away in (1, -1):
            pl.semaphore_signal(barrier, inc=1, device_id=dev(z=at_z(away)), device_id_type=MESH)

    staged = []
    for r in X_ORDER + (0,):
        rows = pl.ds(pl.multiple_of(part(at_x(r), side, co) * PW, PW), PW)
        target = wb.at[0] if r == 0 else wst.at[r - 1]
        for i, w in enumerate((gw, uw)):
            copy = pltpu.make_async_copy(w.at[rows], target.at[:, pl.ds(128 * i, 128)], w_sem.at[r, i])
            copy.start()
            staged.append(copy)

    with jax.named_scope("prepare"):
        to = lax.broadcasted_iota(jnp.int32, (128, 128), 0)
        token = lax.broadcasted_iota(jnp.int32, (128, 128), 1)
        order = (token == 2 * (to % 64) + to // 64).astype(jnp.float32).astype(jnp.bfloat16)
        for i, c in enumerate((gg, ug)):
            loads[i].wait()
            ordered = jnp.dot(order, c[...], preferred_element_type=jnp.float32).astype(jnp.bfloat16)
            for h in range(2):
                cots[0, h, seq, :, 128 * i : 128 * (i + 1)] = ordered[64 * h : 64 * (h + 1)]

        loads[2].wait()
        loads[3].wait()
        total = jnp.zeros((1, PW), jnp.float32)
        for j in range(PARTS):
            v = xin[:, PW * j : PW * (j + 1)].astype(jnp.float32)
            total = total + v * v
        inv_rms = lax.rsqrt(jnp.sum(total, axis=-1, keepdims=True) / D + epsilon)
        for j in range(PARTS):
            v = xin[:, PW * j : PW * (j + 1)].astype(jnp.float32)
            nown[j] = v * inv_rms
            xsend[j, :, :PW] = v
            xsend[j, :, PW:] = jnp.broadcast_to(inv_rms, (1, 128))

    with jax.named_scope("barrier"):
        pl.semaphore_wait(barrier, 31 + 2)
    greet(0, 1)

    sends = []
    with jax.named_scope("start_sends"):
        nrecv[me] = xsend[mine]
        for j in range(1, 16):
            peer, theirs, _ = group_peer(j)
            copy_to(xsend.at[theirs], nrecv.at[me], n_send, n_recv, peer)
        own = cots.at[0, :, seq]
        for r in X_ORDER:
            sends.append(copy_to(own, cots.at[r, :, seq], cx_send.at[r - 1], cx_recv.at[r - 1], dev(x=at_x(r))))
        sends.append(copy_to(own, own, cy_send.at[0], cy_recv.at[0], y_peer))
        sends.append(copy_to(own, own, cc_send.at[0], cc_recv.at[0], core_peer))
        for i in range(8):
            staged[i].wait()
        for k in range(CH):
            rows = pl.ds(CW * k, CW)
            for r in X_ORDER:
                sends.append(
                    copy_to(
                        wst.at[r - 1, rows], wb.at[r, rows], wx_send.at[r - 1, k], wx_recv.at[r - 1, k], dev(x=at_x(r))
                    )
                )

    other = (1 - lo) * 2 + co

    def forward_x(r):
        block = cots.at[r, :, seq]
        wait_bytes(block, cx_recv.at[r - 1])
        sends.append(copy_to(block, block, cy_send.at[r], cy_recv.at[r], y_peer))
        sends.append(copy_to(block, block, cc_send.at[r], cc_recv.at[r], core_peer))

    def forward_y(r):
        block = cots.at[r, :, other]
        wait_bytes(block, cy_recv.at[r])
        sends.append(copy_to(block, block, cc_send.at[4 + r], cc_recv.at[4 + r], core_peer))

    def product(block, k):
        acc = 0.0
        for r in range(NX):
            rows = block(r)
            rows = rows.reshape(rows.shape[0] * 64, 256)
            acc = acc + lax.dot_general(rows, wb[r, CW * k : CW * (k + 1)], NT, preferred_element_type=jnp.float32)
        return acc

    def multiply(l, b, k):
        if k == 0:
            for r in range(NX):
                wait_bytes(cots.at[0, :, 0], cc_recv.at[4 * b + r])
        if b == 0:
            for r in X_ORDER:
                wait_bytes(wb.at[r, pl.ds(CW * k, CW)], wx_recv.at[r - 1, k])
        code, scale = encode(product(lambda r: cots[r, 1 - hi, pl.ds(2 * l, 2)], k))
        psend[k, l, :128] = code
        psend[k, l, 128:] = jnp.broadcast_to(as_row(scale), (16, 128)).astype(jnp.bfloat16)
        sends.append(copy_to(psend.at[k, l], yr.at[k, l], y_send.at[k, b], y_recv.at[k, b], partner))

    def multiply_near(k):
        multiply(lo, 0, k)

    def multiply_far(k):
        multiply(1 - lo, 1, k)

    def multiply_own(k):
        pown[k] = product(lambda r: cots[r, hi], k)

    def add_y(k):
        for b in range(2):
            wait_bytes(yr.at[k, 0], y_recv.at[k, b])
        for l in range(2):
            scale = as_column(yr[k, l, 128:129].astype(jnp.float32), 128)
            half = slice(128 * l, 128 * (l + 1))
            pown[k, half] = pown[k, half] + decode(yr[k, l, :128], scale)
        for b in range(NZ):
            for s in range(4):
                rows = slice(s * 64 + b * 4, s * 64 + b * 4 + 4)
                qz[k, b, 4 * s : 4 * s + 4] = pown[k, rows]
        code, scale = encode(qz[k])
        qc[k] = code
        qs[k] = jnp.sum(scale * eye(16), axis=1, keepdims=True)
        for i, (d, far) in enumerate(Z_RELAY[k % 2]):
            copy_to(qc.at[k, at_z(far)], rrel.at[k, i], zr_send.at[k], zr_recv.at[k], dev(z=at_z(d)))
            copy_to(qs.at[k, at_z(far)], srrel.at[k, i], szr_send.at[k], szr_recv.at[k], dev(z=at_z(d)))
        for i, d in enumerate(Z_DIRECT):
            copy_to(qc.at[k, at_z(d)], rdir.at[k, i], zd_send.at[k], zd_recv.at[k], dev(z=at_z(d)))
            copy_to(qs.at[k, at_z(d)], srdir.at[k, i], szd_send.at[k], szd_recv.at[k], dev(z=at_z(d)))

    def relay(k):
        wait_bytes(rrel.at[k], zr_recv.at[k])
        wait_bytes(srrel.at[k], szr_recv.at[k])
        first = 4 if k % 2 == 0 else -4
        for i, (d, sources) in enumerate(((first, (0, 1, 2, 3)), (-first, (4, 5, 6)))):
            acc = qz[k, at_z(d)]
            for j in sources:
                acc = acc + decode(rrel[k, j], as_column(srrel[k, j], 16))
            code, scale = encode(acc)
            srel[k, i] = code
            ssrel[k, i] = as_row(scale)
            copy_to(srel.at[k, i], r2.at[k, i], z2_send.at[k], z2_recv.at[k], dev(z=at_z(d)))
            copy_to(ssrel.at[k, i], sr2.at[k, i], sz2_send.at[k], sz2_recv.at[k], dev(z=at_z(d)))

    def add_z(k):
        wait_bytes(rdir.at[k], zd_recv.at[k])
        wait_bytes(srdir.at[k], szd_recv.at[k])
        acc = qz[k, z]
        for i in range(6):
            acc = acc + decode(rdir[k, i], as_column(srdir[k, i], 16))
        wait_bytes(r2.at[k], z2_recv.at[k])
        wait_bytes(sr2.at[k], sz2_recv.at[k])
        for i in range(2):
            acc = acc + decode(r2[k, i], as_column(sr2[k, i], 16))
        for i in range(16):
            trow[i, :, CW * k : CW * (k + 1)] = acc[i : i + 1]

    def gather(_):
        pl.semaphore_wait(k_sem.at[0], 2)
        greet(1, 2)
        wait_bytes(nrecv.at[pl.ds(0, 15)], n_recv)
        for i in range(16):
            xf[i : i + 1] = nrecv[i]
        xz[z, :, :PW] = xf[:, :PW].astype(jnp.bfloat16)
        inv = xf[:, PW:]
        high = inv.astype(jnp.bfloat16).astype(jnp.float32)
        middle = (inv - high).astype(jnp.bfloat16).astype(jnp.float32)
        low = inv - high - middle
        lane = lax.broadcasted_iota(jnp.int32, (16, 128), 1)
        split = jnp.where(lane == 0, high, jnp.where(lane == 1, middle, jnp.where(lane == 2, low, 0.0)))
        xz[z, :, PW:] = split.astype(jnp.bfloat16)
        pl.semaphore_wait(k_sem.at[1], 2)
        greet(2, 4)
        for i, d in enumerate((4, -4)):
            copy_to(xz.at[z], xz.at[z], v_send, f_recv.at[i], dev(z=at_z(d)))
        for d in Z_DIRECT:
            copy_to(xz.at[z], xz.at[z], v_send, v_recv, dev(z=at_z(d)))

    def gather_on(_):
        for i, (source, targets) in enumerate(((-4, (1, 2, 3, 4)), (4, (-1, -2, -3)))):
            block = xz.at[at_z(source)]
            wait_bytes(block, f_recv.at[i])
            for d in targets:
                copy_to(block, block, v_send, v_recv, dev(z=at_z(d)))

    def normalize(_):
        wait_bytes(xz.at[pl.ds(0, 13)], v_recv)
        for b in range(NZ):
            block = xz[b].astype(jnp.float32)
            nz[b] = block[:, :PW] * jnp.sum(block[:, PW:], axis=-1, keepdims=True)

    def gain_local(_):
        for k in range(CH):
            cols = slice(CW * k, CW * (k + 1))
            acc = qz[k, 0] * nz[0, :, cols]
            for b in range(1, NZ):
                acc = acc + qz[k, b] * nz[b, :, cols]
            gown[:, cols] = jnp.sum(acc, axis=0, keepdims=True)
        grecv[z] = gown[...]
        pl.semaphore_wait(k_sem.at[2], 2)
        for j in range(1, NZ):
            copy_to(gown, grecv.at[z], g_send, g_recv, dev(z=at_z(j)))

    def gain_far(_):
        wait_bytes(grecv.at[pl.ds(0, NZ - 1)], g_recv)
        acc = grecv[0]
        for i in range(1, NZ):
            acc = acc + grecv[i]
        gsum[...] = acc
        gall[hi, mine] = acc
        for j in range(1, 2 * 16):
            copy_to(gsum, gall.at[hi, mine], a_send, a_recv, plane_peer(j))

    steps = {
        "gather": gather,
        "gather_on": gather_on,
        "normalize": normalize,
        "gain_local": gain_local,
        "gain_far": gain_far,
        "forward_x": forward_x,
        "forward_y": forward_y,
        "near": multiply_near,
        "far": multiply_far,
        "own": multiply_own,
        "add_y": add_y,
        "relay": relay,
        "add_z": add_z,
    }
    for step, k in SCHEDULE:
        with jax.named_scope(f"{step}_{k}"):
            steps[step](k)

    with jax.named_scope("send_rows"):
        rrow[mine] = trow[me]
        for j in range(1, 16):
            peer, _, theirs = group_peer(j)
            copy_to(trow.at[theirs], rrow.at[mine], t_send, t_recv, peer)

    with jax.named_scope("rows"):
        wait_bytes(rrow.at[pl.ds(0, 15)], t_recv)
        total = jnp.zeros((1, PW), jnp.float32)
        for j in range(PARTS):
            total = total + rrow[j] * gain[:, PW * j : PW * (j + 1)] * nown[j]
        inner = jnp.sum(total, axis=-1, keepdims=True) / D
        for j in range(PARTS):
            cols = slice(PW * j, PW * (j + 1))
            scaled = rrow[j] * gain[:, cols]
            out[:, cols] = (inv_rms * (scaled - nown[j] * inner)).astype(jnp.bfloat16)

    with jax.named_scope("gain_all"):
        wait_bytes(gwait, a_recv)
        for j in range(PARTS):
            gout[:, PW * j : PW * (j + 1)] = gall[0, j] + gall[1, j]

    with jax.named_scope("drain"):
        for copy in sends:
            copy.wait_send()
        for k in range(CH):
            wait_bytes(rdir.at[k], zd_send.at[k])
            wait_bytes(rrel.at[k], zr_send.at[k])
            wait_bytes(r2.at[k], z2_send.at[k])
            wait_bytes(srdir.at[k], szd_send.at[k])
            wait_bytes(srrel.at[k], szr_send.at[k])
            wait_bytes(sr2.at[k], sz2_send.at[k])
        wait_bytes(nrecv.at[pl.ds(0, 15)], n_send)
        wait_bytes(xz.at[pl.ds(0, 15)], v_send)
        wait_bytes(rrow.at[pl.ds(0, 15)], t_send)
        wait_bytes(grecv.at[pl.ds(0, NZ - 1)], g_send)
        wait_bytes(gwait, a_send)


def per_device(inputs, norm_gain, gate_grad, up_grad, gate_weight, up_weight):
    f32, bf16 = jnp.float32, jnp.bfloat16
    dma = pltpu.SemaphoreType.DMA
    hbm = pl.BlockSpec(memory_space=pl.ANY)
    vmem = pl.BlockSpec(memory_space=pltpu.VMEM)
    input_grad, gain_grad = pl.pallas_call(
        kernel,
        out_shape=(jax.ShapeDtypeStruct((1, D), bf16), jax.ShapeDtypeStruct((1, D), f32)),
        in_specs=[hbm] * 6,
        out_specs=(vmem, vmem),
        scratch_shapes=[
            pltpu.VMEM((128, 128), bf16),
            pltpu.VMEM((128, 128), bf16),
            pltpu.VMEM((1, D), bf16),
            pltpu.VMEM((1, D), f32),
            pltpu.VMEM((NX, 2, 4, 64, 256), bf16),
            pltpu.VMEM((NX - 1, PW, 256), bf16),
            pltpu.VMEM((NX, PW, 256), bf16),
            pltpu.VMEM((CH, 2, 144, CW), bf16),
            pltpu.VMEM((CH, 256, CW), f32),
            pltpu.VMEM((CH, 2, 144, CW), bf16),
            pltpu.VMEM((CH, NZ, 16, CW), f32),
            pltpu.VMEM((CH, NZ, 16, CW), bf16),
            pltpu.VMEM((CH, NZ, 1, 128), f32),
            pltpu.VMEM((CH, 6, 16, CW), bf16),
            pltpu.VMEM((CH, 7, 16, CW), bf16),
            pltpu.VMEM((CH, 2, 16, CW), bf16),
            pltpu.VMEM((CH, 2, 16, CW), bf16),
            pltpu.VMEM((CH, 6, 1, 128), f32),
            pltpu.VMEM((CH, 7, 1, 128), f32),
            pltpu.VMEM((CH, 2, 1, 128), f32),
            pltpu.VMEM((CH, 2, 1, 128), f32),
            pltpu.VMEM((PARTS, 1, PW), f32),
            pltpu.VMEM((PARTS, 1, XW), f32),
            pltpu.VMEM((16, 1, XW), f32),
            pltpu.VMEM((16, XW), f32),
            pltpu.VMEM((NZ, 16, XW), bf16),
            pltpu.VMEM((NZ, 16, PW), f32),
            pltpu.VMEM((16, 1, PW), f32),
            pltpu.VMEM((PARTS, 1, PW), f32),
            pltpu.VMEM((1, PW), f32),
            pltpu.VMEM((NZ, 1, PW), f32),
            pltpu.VMEM((1, PW), f32),
            pltpu.VMEM((2, PARTS, 1, PW), f32),
            pltpu.VMEM((31, 1, PW), f32),
            pltpu.SemaphoreType.REGULAR((3,)),
            dma((4,)),
            dma((NX, 2)),
            dma((3,)), dma((3,)),
            dma((4,)), dma((4,)),
            dma((8,)), dma((8,)),
            dma((3, CH)), dma((3, CH)),
            dma((CH, 2)), dma((CH, 2)),
            dma((CH,)), dma((CH,)),
            dma((CH,)), dma((CH,)),
            dma((CH,)), dma((CH,)),
            dma((CH,)), dma((CH,)),
            dma((CH,)), dma((CH,)),
            dma((CH,)), dma((CH,)),
            dma, dma, dma, dma, dma((2,)),
            dma, dma, dma, dma, dma, dma,
        ],
        compiler_params=pltpu.CompilerParams(collective_id=0, has_side_effects=True, vmem_limit_bytes=VMEM_GRANT),
    )(
        gate_weight,
        up_weight,
        gate_grad[0],
        up_grad[0],
        inputs[0],
        norm_gain.reshape(1, D),
    )
    return (input_grad[None], gain_grad.reshape(D))


def solution(mesh):
    finer = Mesh(mesh.devices.reshape(2, 2, NZ, NX, 2), ("dp_0", "dp_1", "tp_0", "tp_1", "tp_2"))
    return jax.shard_map(
        per_device,
        mesh=finer,
        in_specs=(P(DP, TP, None), P(), P(DP, None, TP), P(DP, None, TP), P(None, TP), P(None, TP)),
        out_specs=(P(DP, TP, None), P()),
        check_vma=False,
    )
```

```python
import math

import jax
import jax.numpy as jnp
from jax import lax
from jax.experimental import pallas as pl
from jax.experimental.pallas import tpu as pltpu
from jax.sharding import Mesh
from jax.sharding import PartitionSpec as P

TP = ("tp_0", "tp_1", "tp_2")
DP = ("dp_0", "dp_1")
MESH = pl.DeviceIdType.MESH

epsilon = 1e-05

D = 8192
NX = 4
NZ = 16
PARTS = 16
PW = D // PARTS
CH = 4
CW = PW // CH
X_ORDER = (1, 3, 2)
VMEM_GRANT = 55150 * 1024
LEVELS = 240.0
UNIT = 512
BLOCK = 9
XBLOCK = 33
MIDDLE = 120.0
Z_DIRECT = (1, 2, 3, -1, -2, -3)
Z_UP, Z_DOWN = ((1, 5), (2, 6), (3, 7)), ((-1, -5), (-2, -6), (-3, -7))
Z_RELAY = (Z_UP + ((4, 8),) + Z_DOWN, Z_DOWN + ((-4, -8),) + Z_UP)
XW = PW + 128
SCHEDULE = (
    ("gather", 0),
    ("forward_x", 1),
    ("forward_x", 3),
    ("forward_x", 2),
    ("forward_y", 0),
    ("forward_y", 1),
    ("near", 0),
    ("forward_y", 3),
    ("forward_y", 2),
    ("far", 0),
    ("own", 0),
    ("gather_on", 0),
    ("near", 1),
    ("far", 1),
    ("own", 1),
    ("add_y", 0),
    ("near", 2),
    ("far", 2),
    ("own", 2),
    ("near", 3),
    ("far", 3),
    ("own", 3),
    ("add_y", 1),
    ("add_y", 2),
    ("relay", 0),
    ("add_y", 3),
    ("normalize", 0),
    ("gain_local", 0),
    ("relay", 1),
    ("relay", 2),
    ("relay", 3),
    ("add_z", 0),
    ("add_z", 1),
    ("add_z", 2),
    ("gain_far", 0),
    ("add_z", 3),
)
NT = (((1,), (1,)), ((), ()))


def encode(v):
    size = jnp.abs(v)
    scale = jnp.maximum(jnp.max(size, axis=-1, keepdims=True) * 1.001, 1e-30)
    t = size * (LEVELS / scale)
    whole = jnp.floor(t)
    code = jnp.exp2(whole - MIDDLE) * (1.0 + (t - whole))
    return jnp.where(v < 0.0, -code, code).astype(jnp.bfloat16), scale


def decode(code, scale):
    code = code.astype(jnp.float32)
    size = jnp.abs(code)
    power = jnp.floor(jnp.log2(size))
    t = size * jnp.exp2(-power) + (power + (MIDDLE - 1.0))
    return jnp.where(code < 0.0, -t, t) * (scale * (1.0 / LEVELS))


def eye(rows):
    row = lax.broadcasted_iota(jnp.int32, (rows, 128), 0)
    lane = lax.broadcasted_iota(jnp.int32, (rows, 128), 1)
    return (row == lane).astype(jnp.float32)


def as_row(column):
    return jnp.sum(column * eye(column.shape[0]), axis=0, keepdims=True)


def as_column(row, rows):
    return jnp.sum(row * eye(rows), axis=-1, keepdims=True)


def wait_bytes(ref, sem):
    pltpu.make_async_copy(ref, ref, sem).wait()


def kernel(
    gw, uw, gg_in, ug_in, x_in, gain_in, out, gout,
    gug, xin, gain, cots, wst, wb, psend, spsend, pown, yr, syr, qz, qc, qs, rdir, rrel, srel, r2, srdir, srrel, ssrel, sr2, nown, xsend, nrecv, xf, xz, iz, nz, trow, rrow, gown, grecv, gsum, gall, units,
    k_sem, in_sem, w_sem, send_sem, cx_recv, cy_recv, cc_recv, wx_recv, y_recv, zr_recv, zd_recv, n_recv, v_recv, f_recv,
    t_recv, g_recv, a_recv,
):
    lo, co = lax.axis_index("dp_0"), lax.axis_index("dp_1")
    z, x, hi = lax.axis_index("tp_0"), lax.axis_index("tp_1"), lax.axis_index("tp_2")

    def dev(lo=lo, co=co, z=z, x=x, hi=hi):
        return {"dp_0": lo, "dp_1": co, "tp_0": z, "tp_1": x, "tp_2": hi}

    def at_x(r):
        return lax.rem(x + r, NX)

    def at_z(d):
        return lax.rem(z + (d + NZ), NZ)

    side = lax.rem(lo + hi, 2)

    def part(x, side, co):
        return (x * 2 + side) * 2 + co

    def group_peer(j):
        dx, dlo, dco = j // 4, (j // 2) % 2, j % 2
        px, plo, pco = lax.rem(x + dx, NX), lax.rem(lo + dlo, 2), lax.rem(co + dco, 2)
        return dev(lo=plo, co=pco, x=px), part(px, lax.rem(plo + hi, 2), pco), (plo * 2 + pco) * NX + px

    def plane_peer(j):
        dx, dlo, dco, dhi = j // 8, (j // 4) % 2, (j // 2) % 2, j % 2
        return dev(lo=lax.rem(lo + dlo, 2), co=lax.rem(co + dco, 2), x=lax.rem(x + dx, NX), hi=lax.rem(hi + dhi, 2))

    def greet(step, d):
        for away in (d, -d):
            pl.semaphore_signal(k_sem.at[step], inc=1, device_id=dev(z=at_z(away)), device_id_type=MESH)

    mine = part(x, side, co)
    me = (lo * 2 + co) * NX + x
    seq = lo * 2 + co
    y_peer = dev(lo=1 - lo)
    core_peer = dev(co=1 - co)
    partner = dev(lo=1 - lo, hi=1 - hi)

    sent = []

    def copy_to(src, dst, recv, device):
        pltpu.make_async_remote_copy(
            src_ref=src, dst_ref=dst, send_sem=send_sem, recv_sem=recv, device_id=device, device_id_type=MESH
        ).start()
        sent.append(math.prod(src.shape) * src.dtype.itemsize // UNIT)

    def wait_units(count, sem):
        wait_bytes(units.at[pl.ds(0, count)], sem)

    loads = []
    pairs = ((gg_in, gug.at[0]), (ug_in, gug.at[1]), (x_in, xin), (gain_in, gain))
    for (src, dst), i in zip(pairs, (0, 0, 1, 2)):
        loads.append(pltpu.make_async_copy(src, dst, in_sem.at[i]))
        loads[-1].start()
    with jax.named_scope("signals"):
        barrier = pltpu.get_barrier_semaphore()
        for j in range(1, 2 * 16):
            pl.semaphore_signal(barrier, inc=1, device_id=plane_peer(j), device_id_type=MESH)
        for away in (1, -1):
            pl.semaphore_signal(barrier, inc=1, device_id=dev(z=at_z(away)), device_id_type=MESH)

    for r in X_ORDER + (0,):
        rows = pl.ds(pl.multiple_of(part(at_x(r), side, co) * PW, PW), PW)
        target = wb.at[0] if r == 0 else wst.at[r - 1]
        for i, w in enumerate((gw, uw)):
            pltpu.make_async_copy(w.at[rows], target.at[:, pl.ds(128 * i, 128)], w_sem).start()

    with jax.named_scope("prepare"):
        to = lax.broadcasted_iota(jnp.int32, (128, 128), 0)
        token = lax.broadcasted_iota(jnp.int32, (128, 128), 1)
        order = (token == 2 * (to % 64) + to // 64).astype(jnp.float32).astype(jnp.bfloat16)
        wait_bytes(gug, in_sem.at[0])
        for i in range(2):
            ordered = jnp.dot(order, gug[i], preferred_element_type=jnp.float32).astype(jnp.bfloat16)
            for h in range(2):
                cots[0, h, seq, :, 128 * i : 128 * (i + 1)] = ordered[64 * h : 64 * (h + 1)]

        loads[2].wait()
        loads[3].wait()
        total = jnp.zeros((1, PW), jnp.float32)
        for j in range(PARTS):
            v = xin[:, PW * j : PW * (j + 1)].astype(jnp.float32)
            total = total + v * v
        inv_rms = lax.rsqrt(jnp.sum(total, axis=-1, keepdims=True) / D + epsilon)
        for j in range(PARTS):
            v = xin[:, PW * j : PW * (j + 1)].astype(jnp.float32)
            nown[j] = v * inv_rms
            xsend[j, :, :PW] = v
            xsend[j, :, PW:] = jnp.broadcast_to(inv_rms, (1, 128))

    with jax.named_scope("barrier"):
        pl.semaphore_wait(barrier, 31 + 2)
    greet(0, 1)

    with jax.named_scope("start_sends"):
        nrecv[me] = xsend[mine]
        for j in range(1, 16):
            peer, theirs, _ = group_peer(j)
            copy_to(xsend.at[theirs], nrecv.at[me], n_recv, peer)
        own = cots.at[0, :, seq]
        for r in X_ORDER:
            copy_to(own, cots.at[r, :, seq], cx_recv.at[r - 1], dev(x=at_x(r)))
        copy_to(own, own, cy_recv.at[0], y_peer)
        copy_to(own, own, cc_recv.at[0], core_peer)
        wait_bytes(wb, w_sem)
        for k in range(CH):
            rows = pl.ds(CW * k, CW)
            for r in X_ORDER:
                copy_to(wst.at[r - 1, rows], wb.at[r, rows], wx_recv.at[k], dev(x=at_x(r)))

    other = (1 - lo) * 2 + co

    def forward_x(r):
        block = cots.at[r, :, seq]
        wait_bytes(block, cx_recv.at[r - 1])
        copy_to(block, block, cy_recv.at[r], y_peer)
        copy_to(block, block, cc_recv.at[0], core_peer)

    def forward_y(r):
        block = cots.at[r, :, other]
        wait_bytes(block, cy_recv.at[r])
        copy_to(block, block, cc_recv.at[1], core_peer)

    def product(block, k):
        acc = 0.0
        for r in range(NX):
            rows = block(r)
            rows = rows.reshape(rows.shape[0] * 64, 256)
            acc = acc + lax.dot_general(rows, wb[r, CW * k : CW * (k + 1)], NT, preferred_element_type=jnp.float32)
        return acc

    def multiply(l, b, k):
        if k == 0:
            wait_bytes(cots.at[:, :, 0], cc_recv.at[b])
        if b == 0:
            wait_bytes(wb.at[pl.ds(0, 3), pl.ds(0, CW)], wx_recv.at[k])
        code, scale = encode(product(lambda r: cots[r, 1 - hi, pl.ds(2 * l, 2)], k))
        psend[k, l] = code
        spsend[k, l] = as_row(scale)
        copy_to(psend.at[k, l], yr.at[k, l], y_recv.at[k], partner)
        copy_to(spsend.at[k, l], syr.at[k, l], y_recv.at[k], partner)

    def multiply_near(k):
        multiply(lo, 0, k)

    def multiply_far(k):
        multiply(1 - lo, 1, k)

    def multiply_own(k):
        pown[k] = product(lambda r: cots[r, hi], k)

    def add_y(k):
        wait_units(2 * (64 + 1), y_recv.at[k])
        for l in range(2):
            scale = as_column(syr[k, l], 128)
            half = slice(128 * l, 128 * (l + 1))
            pown[k, half] = pown[k, half] + decode(yr[k, l], scale)
        for b in range(NZ):
            for s in range(4):
                rows = slice(s * 64 + b * 4, s * 64 + b * 4 + 4)
                qz[k, b, 4 * s : 4 * s + 4] = pown[k, rows]
        code, scale = encode(qz[k])
        qc[k] = code
        qs[k] = jnp.sum(scale * eye(16), axis=1, keepdims=True)
        for i, (d, far) in enumerate(Z_RELAY[k % 2]):
            copy_to(qc.at[k, at_z(far)], rrel.at[k, i], zr_recv.at[k], dev(z=at_z(d)))
            copy_to(qs.at[k, at_z(far)], srrel.at[k, i], zr_recv.at[k], dev(z=at_z(d)))
        for i, d in enumerate(Z_DIRECT):
            copy_to(qc.at[k, at_z(d)], rdir.at[k, i], zd_recv.at[k], dev(z=at_z(d)))
            copy_to(qs.at[k, at_z(d)], srdir.at[k, i], zd_recv.at[k], dev(z=at_z(d)))

    def relay(k):
        wait_units(7 * BLOCK, zr_recv.at[k])
        first = 4 if k % 2 == 0 else -4
        for i, (d, sources) in enumerate(((first, (0, 1, 2, 3)), (-first, (4, 5, 6)))):
            acc = qz[k, at_z(d)]
            for j in sources:
                acc = acc + decode(rrel[k, j], as_column(srrel[k, j], 16))
            code, scale = encode(acc)
            srel[k, i] = code
            ssrel[k, i] = as_row(scale)
            copy_to(srel.at[k, i], r2.at[k, i], zd_recv.at[k], dev(z=at_z(d)))
            copy_to(ssrel.at[k, i], sr2.at[k, i], zd_recv.at[k], dev(z=at_z(d)))

    def add_z(k):
        wait_units(8 * BLOCK, zd_recv.at[k])
        acc = qz[k, z]
        for i in range(6):
            acc = acc + decode(rdir[k, i], as_column(srdir[k, i], 16))
        for i in range(2):
            acc = acc + decode(r2[k, i], as_column(sr2[k, i], 16))
        for i in range(16):
            trow[i, :, CW * k : CW * (k + 1)] = acc[i : i + 1]

    def share(b, sem, d):
        for ref in (xz, iz):
            copy_to(ref.at[b], ref.at[b], sem, dev(z=at_z(d)))

    def gather(_):
        pl.semaphore_wait(k_sem.at[0], 2)
        greet(1, 2)
        wait_bytes(nrecv.at[pl.ds(0, 15)], n_recv)
        for i in range(16):
            xf[i : i + 1] = nrecv[i]
        xz[z] = xf[:, :PW].astype(jnp.bfloat16)
        iz[z] = as_row(xf[:, PW : PW + 1])
        pl.semaphore_wait(k_sem.at[1], 2)
        greet(2, 4)
        for i, d in enumerate((4, -4)):
            share(z, f_recv.at[i], d)
        for d in Z_DIRECT:
            share(z, v_recv, d)

    def gather_on(_):
        for i, (source, targets) in enumerate(((-4, (1, 2, 3, 4)), (4, (-1, -2, -3)))):
            wait_units(XBLOCK, f_recv.at[i])
            for d in targets:
                share(at_z(source), v_recv, d)

    def normalize(_):
        wait_units(13 * XBLOCK, v_recv)
        for b in range(NZ):
            nz[b] = xz[b].astype(jnp.float32) * as_column(iz[b], 16)

    def gain_local(_):
        for k in range(CH):
            cols = slice(CW * k, CW * (k + 1))
            acc = qz[k, 0] * nz[0, :, cols]
            for b in range(1, NZ):
                acc = acc + qz[k, b] * nz[b, :, cols]
            gown[:, cols] = jnp.sum(acc, axis=0, keepdims=True)
        grecv[z] = gown[...]
        pl.semaphore_wait(k_sem.at[2], 2)
        for j in range(1, NZ):
            copy_to(gown, grecv.at[z], g_recv, dev(z=at_z(j)))

    def gain_far(_):
        wait_bytes(grecv.at[pl.ds(0, NZ - 1)], g_recv)
        acc = grecv[0]
        for i in range(1, NZ):
            acc = acc + grecv[i]
        gsum[...] = acc
        gall[hi, mine] = acc
        for j in range(1, 2 * 16):
            copy_to(gsum, gall.at[hi, mine], a_recv, plane_peer(j))

    steps = {
        "gather": gather,
        "gather_on": gather_on,
        "normalize": normalize,
        "gain_local": gain_local,
        "gain_far": gain_far,
        "forward_x": forward_x,
        "forward_y": forward_y,
        "near": multiply_near,
        "far": multiply_far,
        "own": multiply_own,
        "add_y": add_y,
        "relay": relay,
        "add_z": add_z,
    }
    for step, k in SCHEDULE:
        with jax.named_scope(f"{step}_{k}"):
            steps[step](k)

    with jax.named_scope("send_rows"):
        rrow[mine] = trow[me]
        for j in range(1, 16):
            peer, _, theirs = group_peer(j)
            copy_to(trow.at[theirs], rrow.at[mine], t_recv, peer)

    with jax.named_scope("rows"):
        wait_bytes(rrow.at[pl.ds(0, 15)], t_recv)
        total = jnp.zeros((1, PW), jnp.float32)
        for j in range(PARTS):
            total = total + rrow[j] * gain[:, PW * j : PW * (j + 1)] * nown[j]
        inner = jnp.sum(total, axis=-1, keepdims=True) / D
        for j in range(PARTS):
            cols = slice(PW * j, PW * (j + 1))
            scaled = rrow[j] * gain[:, cols]
            out[:, cols] = (inv_rms * (scaled - nown[j] * inner)).astype(jnp.bfloat16)

    with jax.named_scope("gain_all"):
        wait_units(31 * PW * 4 // UNIT, a_recv)
        for j in range(PARTS):
            gout[:, PW * j : PW * (j + 1)] = gall[0, j] + gall[1, j]

    with jax.named_scope("drain"):
        wait_units(sum(sent), send_sem)


def per_device(inputs, norm_gain, gate_grad, up_grad, gate_weight, up_weight):
    f32, bf16 = jnp.float32, jnp.bfloat16
    dma = pltpu.SemaphoreType.DMA
    hbm = pl.BlockSpec(memory_space=pl.ANY)
    vmem = pl.BlockSpec(memory_space=pltpu.VMEM)
    input_grad, gain_grad = pl.pallas_call(
        kernel,
        out_shape=(jax.ShapeDtypeStruct((1, D), bf16), jax.ShapeDtypeStruct((1, D), f32)),
        in_specs=[hbm] * 6,
        out_specs=(vmem, vmem),
        scratch_shapes=[
            pltpu.VMEM((2, 128, 128), bf16),
            pltpu.VMEM((1, D), bf16),
            pltpu.VMEM((1, D), f32),
            pltpu.VMEM((NX, 2, 4, 64, 256), bf16),
            pltpu.VMEM((NX - 1, PW, 256), bf16),
            pltpu.VMEM((NX, PW, 256), bf16),
            pltpu.VMEM((CH, 2, 128, CW), bf16),
            pltpu.VMEM((CH, 2, 1, 128), f32),
            pltpu.VMEM((CH, 256, CW), f32),
            pltpu.VMEM((CH, 2, 128, CW), bf16),
            pltpu.VMEM((CH, 2, 1, 128), f32),
            pltpu.VMEM((CH, NZ, 16, CW), f32),
            pltpu.VMEM((CH, NZ, 16, CW), bf16),
            pltpu.VMEM((CH, NZ, 1, 128), f32),
            pltpu.VMEM((CH, 6, 16, CW), bf16),
            pltpu.VMEM((CH, 7, 16, CW), bf16),
            pltpu.VMEM((CH, 2, 16, CW), bf16),
            pltpu.VMEM((CH, 2, 16, CW), bf16),
            pltpu.VMEM((CH, 6, 1, 128), f32),
            pltpu.VMEM((CH, 7, 1, 128), f32),
            pltpu.VMEM((CH, 2, 1, 128), f32),
            pltpu.VMEM((CH, 2, 1, 128), f32),
            pltpu.VMEM((PARTS, 1, PW), f32),
            pltpu.VMEM((PARTS, 1, XW), f32),
            pltpu.VMEM((16, 1, XW), f32),
            pltpu.VMEM((16, XW), f32),
            pltpu.VMEM((NZ, 16, PW), bf16),
            pltpu.VMEM((NZ, 1, 128), f32),
            pltpu.VMEM((NZ, 16, PW), f32),
            pltpu.VMEM((16, 1, PW), f32),
            pltpu.VMEM((PARTS, 1, PW), f32),
            pltpu.VMEM((1, PW), f32),
            pltpu.VMEM((NZ, 1, PW), f32),
            pltpu.VMEM((1, PW), f32),
            pltpu.VMEM((2, PARTS, 1, PW), f32),
            pltpu.VMEM((6000, 1, 128), f32),
            pltpu.SemaphoreType.REGULAR((3,)),
            dma((3,)),
            dma, dma,
            dma((3,)), dma((4,)), dma((2,)),
            dma((CH,)), dma((CH,)),
            dma((CH,)), dma((CH,)),
            dma, dma, dma((2,)),
            dma, dma, dma,
        ],
        compiler_params=pltpu.CompilerParams(collective_id=0, has_side_effects=True, vmem_limit_bytes=VMEM_GRANT),
    )(
        gate_weight,
        up_weight,
        gate_grad[0],
        up_grad[0],
        inputs[0],
        norm_gain.reshape(1, D),
    )
    return (input_grad[None], gain_grad.reshape(D))


def solution(mesh):
    finer = Mesh(mesh.devices.reshape(2, 2, NZ, NX, 2), ("dp_0", "dp_1", "tp_0", "tp_1", "tp_2"))
    return jax.shard_map(
        per_device,
        mesh=finer,
        in_specs=(P(DP, TP, None), P(), P(DP, None, TP), P(DP, None, TP), P(None, TP), P(None, TP)),
        out_specs=(P(DP, TP, None), P()),
        check_vma=False,
    )
```

```python
import math

import jax
import jax.numpy as jnp
from jax import lax
from jax.experimental import pallas as pl
from jax.experimental.pallas import tpu as pltpu
from jax.sharding import Mesh
from jax.sharding import PartitionSpec as P

TP = ("tp_0", "tp_1", "tp_2")
DP = ("dp_0", "dp_1")
MESH = pl.DeviceIdType.MESH

epsilon = 1e-05

D = 8192
NX = 4
NZ = 16
PARTS = 16
PW = D // PARTS
CH = 4
CW = PW // CH
X_ORDER = (1, 3, 2)
VMEM_GRANT = 55150 * 1024
LEVELS = 240.0
UNIT = 512
BLOCK = 9
XBLOCK = 33
MIDDLE = 120.0
Z_DIRECT = (1, 2, 3, -1, -2, -3)
Z_UP, Z_DOWN = ((1, 5), (2, 6), (3, 7)), ((-1, -5), (-2, -6), (-3, -7))
Z_RELAY = (Z_UP + ((4, 8),) + Z_DOWN, Z_DOWN + ((-4, -8),) + Z_UP)
XW = PW + 128
SCHEDULE = (
    ("forward_x", 1),
    ("forward_x", 3),
    ("forward_x", 2),
    ("forward_y", 0),
    ("forward_y", 1),
    ("gather", 0),
    ("forward_y", 3),
    ("near", 0),
    ("forward_y", 2),
    ("far", 0),
    ("own", 0),
    ("near", 1),
    ("far", 1),
    ("gather_on", 0),
    ("own", 1),
    ("add_y", 0),
    ("near", 2),
    ("far", 2),
    ("own", 2),
    ("near", 3),
    ("far", 3),
    ("own", 3),
    ("add_y", 1),
    ("add_y", 2),
    ("relay", 0),
    ("add_y", 3),
    ("normalize", 0),
    ("gain_local", 0),
    ("relay", 1),
    ("relay", 2),
    ("relay", 3),
    ("add_z", 0),
    ("add_z", 1),
    ("add_z", 2),
    ("gain_far", 0),
    ("add_z", 3),
)
NT = (((1,), (1,)), ((), ()))


def encode(v):
    size = jnp.abs(v)
    scale = jnp.maximum(jnp.max(size, axis=-1, keepdims=True) * 1.001, 1e-30)
    t = size * (LEVELS / scale)
    whole = jnp.floor(t)
    code = jnp.exp2(whole - MIDDLE) * (1.0 + (t - whole))
    return jnp.where(v < 0.0, -code, code).astype(jnp.bfloat16), scale


def decode(code, scale):
    code = code.astype(jnp.float32)
    size = jnp.abs(code)
    power = jnp.floor(jnp.log2(size))
    t = size * jnp.exp2(-power) + (power + (MIDDLE - 1.0))
    return jnp.where(code < 0.0, -t, t) * (scale * (1.0 / LEVELS))


def eye(rows):
    row = lax.broadcasted_iota(jnp.int32, (rows, 128), 0)
    lane = lax.broadcasted_iota(jnp.int32, (rows, 128), 1)
    return (row == lane).astype(jnp.float32)


def as_row(column):
    return jnp.sum(column * eye(column.shape[0]), axis=0, keepdims=True)


def as_column(row, rows):
    return jnp.sum(row * eye(rows), axis=-1, keepdims=True)


def wait_bytes(ref, sem):
    pltpu.make_async_copy(ref, ref, sem).wait()


def kernel(
    gw, uw, gg_in, ug_in, x_in, gain_in, out, gout,
    gug, xin, gain, cots, wst, wb, psend, spsend, pown, yr, syr, qz, qc, qs, rdir, rrel, srel, r2, srdir, srrel, ssrel, sr2, nown, xsend, nrecv, xf, xz, iz, nz, trow, rrow, gown, grecv, gsum, gall, units,
    k_sem, m_sem, in_sem, w_sem, send_sem, cx_recv, cy_recv, cc_recv, wx_recv, y_recv, zr_recv, zd_recv, n_recv, v_recv, f_recv,
    t_recv, g_recv, a_recv,
):
    lo, co = lax.axis_index("dp_0"), lax.axis_index("dp_1")
    z, x, hi = lax.axis_index("tp_0"), lax.axis_index("tp_1"), lax.axis_index("tp_2")

    def dev(lo=lo, co=co, z=z, x=x, hi=hi):
        return {"dp_0": lo, "dp_1": co, "tp_0": z, "tp_1": x, "tp_2": hi}

    def at_x(r):
        return lax.rem(x + r, NX)

    def at_z(d):
        return lax.rem(z + (d + NZ), NZ)

    side = lax.rem(lo + hi, 2)

    def part(x, side, co):
        return (x * 2 + side) * 2 + co

    def group_peer(j):
        dx, dlo, dco = j // 4, (j // 2) % 2, j % 2
        px, plo, pco = lax.rem(x + dx, NX), lax.rem(lo + dlo, 2), lax.rem(co + dco, 2)
        return dev(lo=plo, co=pco, x=px), part(px, lax.rem(plo + hi, 2), pco), (plo * 2 + pco) * NX + px

    def plane_peer(j):
        dx, dlo, dco, dhi = j // 8, (j // 4) % 2, (j // 2) % 2, j % 2
        return dev(lo=lax.rem(lo + dlo, 2), co=lax.rem(co + dco, 2), x=lax.rem(x + dx, NX), hi=lax.rem(hi + dhi, 2))

    def greet(step, d):
        for away in (d, -d):
            pl.semaphore_signal(k_sem.at[step], inc=1, device_id=dev(z=at_z(away)), device_id_type=MESH)

    mine = part(x, side, co)
    me = (lo * 2 + co) * NX + x
    seq = lo * 2 + co
    y_peer = dev(lo=1 - lo)
    core_peer = dev(co=1 - co)
    partner = dev(lo=1 - lo, hi=1 - hi)

    sent = []

    def copy_to(src, dst, recv, device):
        pltpu.make_async_remote_copy(
            src_ref=src, dst_ref=dst, send_sem=send_sem, recv_sem=recv, device_id=device, device_id_type=MESH
        ).start()
        sent.append(math.prod(src.shape) * src.dtype.itemsize // UNIT)

    def wait_units(count, sem):
        wait_bytes(units.at[pl.ds(0, count)], sem)

    loads = []
    pairs = ((gg_in, gug.at[0]), (ug_in, gug.at[1]), (x_in, xin), (gain_in, gain))
    for (src, dst), i in zip(pairs, (0, 0, 1, 2)):
        loads.append(pltpu.make_async_copy(src, dst, in_sem.at[i]))
        loads[-1].start()
    with jax.named_scope("signals"):
        barrier = pltpu.get_barrier_semaphore()
        near = [dev(x=at_x(r)) for r in X_ORDER] + [dev(z=at_z(1)), dev(z=at_z(-1)), y_peer, core_peer, partner]
        for peer in near:
            pl.semaphore_signal(barrier, inc=1, device_id=peer, device_id_type=MESH)

    for r in X_ORDER + (0,):
        rows = pl.ds(pl.multiple_of(part(at_x(r), side, co) * PW, PW), PW)
        target = wb.at[0] if r == 0 else wst.at[r - 1]
        for i, w in enumerate((gw, uw)):
            pltpu.make_async_copy(w.at[rows], target.at[:, pl.ds(128 * i, 128)], w_sem).start()

    with jax.named_scope("prepare"):
        to = lax.broadcasted_iota(jnp.int32, (128, 128), 0)
        token = lax.broadcasted_iota(jnp.int32, (128, 128), 1)
        order = (token == 2 * (to % 64) + to // 64).astype(jnp.float32).astype(jnp.bfloat16)
        wait_bytes(gug, in_sem.at[0])
        for i in range(2):
            ordered = jnp.dot(order, gug[i], preferred_element_type=jnp.float32).astype(jnp.bfloat16)
            for h in range(2):
                cots[0, h, seq, :, 128 * i : 128 * (i + 1)] = ordered[64 * h : 64 * (h + 1)]

    with jax.named_scope("barrier"):
        pl.semaphore_wait(barrier, len(near))

    def meet(step, *peers):
        for peer in peers:
            pl.semaphore_signal(m_sem.at[step], inc=1, device_id=peer, device_id_type=MESH)

    meet(0, y_peer, core_peer)
    greet(0, 1)

    with jax.named_scope("start_cots"):
        own = cots.at[0, :, seq]
        for r in X_ORDER:
            copy_to(own, cots.at[r, :, seq], cx_recv.at[r - 1], dev(x=at_x(r)))
        copy_to(own, own, cy_recv.at[0], y_peer)
        copy_to(own, own, cc_recv.at[0], core_peer)
        loads[2].wait()
        loads[3].wait()
        total = jnp.zeros((1, PW), jnp.float32)
        for j in range(PARTS):
            v = xin[:, PW * j : PW * (j + 1)].astype(jnp.float32)
            total = total + v * v
        inv_rms = lax.rsqrt(jnp.sum(total, axis=-1, keepdims=True) / D + epsilon)
        for j in range(PARTS):
            v = xin[:, PW * j : PW * (j + 1)].astype(jnp.float32)
            nown[j] = v * inv_rms
            xsend[j, :, :PW] = v
            xsend[j, :, PW:] = jnp.broadcast_to(inv_rms, (1, 128))
    with jax.named_scope("meet"):
        pl.semaphore_wait(m_sem.at[0], 2)
        meet(1, y_peer)
        pl.semaphore_wait(m_sem.at[1], 1)
        pl.semaphore_wait(k_sem.at[0], 2)
        greet(1, 2)
    with jax.named_scope("start_sends"):
        nrecv[me] = xsend[mine]
        for j in range(1, 16):
            peer, theirs, _ = group_peer(j)
            copy_to(xsend.at[theirs], nrecv.at[me], n_recv, peer)
        wait_bytes(wb, w_sem)
        for k in range(CH):
            rows = pl.ds(CW * k, CW)
            for r in X_ORDER:
                copy_to(wst.at[r - 1, rows], wb.at[r, rows], wx_recv.at[k], dev(x=at_x(r)))

    other = (1 - lo) * 2 + co

    def forward_x(r):
        block = cots.at[r, :, seq]
        wait_bytes(block, cx_recv.at[r - 1])
        copy_to(block, block, cy_recv.at[r], y_peer)
        copy_to(block, block, cc_recv.at[0], core_peer)

    def forward_y(r):
        block = cots.at[r, :, other]
        wait_bytes(block, cy_recv.at[r])
        copy_to(block, block, cc_recv.at[1], core_peer)

    def product(block, k):
        acc = 0.0
        for r in range(NX):
            rows = block(r)
            rows = rows.reshape(rows.shape[0] * 64, 256)
            acc = acc + lax.dot_general(rows, wb[r, CW * k : CW * (k + 1)], NT, preferred_element_type=jnp.float32)
        return acc

    def multiply(l, b, k):
        if k == 0:
            wait_bytes(cots.at[:, :, 0], cc_recv.at[b])
        if b == 0:
            wait_bytes(wb.at[pl.ds(0, 3), pl.ds(0, CW)], wx_recv.at[k])
        code, scale = encode(product(lambda r: cots[r, 1 - hi, pl.ds(2 * l, 2)], k))
        psend[k, l] = code
        spsend[k, l] = as_row(scale)
        copy_to(psend.at[k, l], yr.at[k, l], y_recv.at[k], partner)
        copy_to(spsend.at[k, l], syr.at[k, l], y_recv.at[k], partner)

    def multiply_near(k):
        multiply(lo, 0, k)

    def multiply_far(k):
        multiply(1 - lo, 1, k)

    def multiply_own(k):
        pown[k] = product(lambda r: cots[r, hi], k)

    def add_y(k):
        wait_units(2 * (64 + 1), y_recv.at[k])
        for l in range(2):
            scale = as_column(syr[k, l], 128)
            half = slice(128 * l, 128 * (l + 1))
            pown[k, half] = pown[k, half] + decode(yr[k, l], scale)
        for b in range(NZ):
            for s in range(4):
                rows = slice(s * 64 + b * 4, s * 64 + b * 4 + 4)
                qz[k, b, 4 * s : 4 * s + 4] = pown[k, rows]
        code, scale = encode(qz[k])
        qc[k] = code
        qs[k] = jnp.sum(scale * eye(16), axis=1, keepdims=True)
        for i, (d, far) in enumerate(Z_RELAY[k % 2]):
            copy_to(qc.at[k, at_z(far)], rrel.at[k, i], zr_recv.at[k], dev(z=at_z(d)))
            copy_to(qs.at[k, at_z(far)], srrel.at[k, i], zr_recv.at[k], dev(z=at_z(d)))
        for i, d in enumerate(Z_DIRECT):
            copy_to(qc.at[k, at_z(d)], rdir.at[k, i], zd_recv.at[k], dev(z=at_z(d)))
            copy_to(qs.at[k, at_z(d)], srdir.at[k, i], zd_recv.at[k], dev(z=at_z(d)))

    def relay(k):
        wait_units(7 * BLOCK, zr_recv.at[k])
        first = 4 if k % 2 == 0 else -4
        for i, (d, sources) in enumerate(((first, (0, 1, 2, 3)), (-first, (4, 5, 6)))):
            acc = qz[k, at_z(d)]
            for j in sources:
                acc = acc + decode(rrel[k, j], as_column(srrel[k, j], 16))
            code, scale = encode(acc)
            srel[k, i] = code
            ssrel[k, i] = as_row(scale)
            copy_to(srel.at[k, i], r2.at[k, i], zd_recv.at[k], dev(z=at_z(d)))
            copy_to(ssrel.at[k, i], sr2.at[k, i], zd_recv.at[k], dev(z=at_z(d)))

    def add_z(k):
        wait_units(8 * BLOCK, zd_recv.at[k])
        acc = qz[k, z]
        for i in range(6):
            acc = acc + decode(rdir[k, i], as_column(srdir[k, i], 16))
        for i in range(2):
            acc = acc + decode(r2[k, i], as_column(sr2[k, i], 16))
        for i in range(16):
            trow[i, :, CW * k : CW * (k + 1)] = acc[i : i + 1]

    def share(b, sem, d):
        for ref in (xz, iz):
            copy_to(ref.at[b], ref.at[b], sem, dev(z=at_z(d)))

    def gather(_):
        wait_bytes(nrecv.at[pl.ds(0, 15)], n_recv)
        for i in range(16):
            xf[i : i + 1] = nrecv[i]
        xz[z] = xf[:, :PW].astype(jnp.bfloat16)
        iz[z] = as_row(xf[:, PW : PW + 1])
        pl.semaphore_wait(k_sem.at[1], 2)
        greet(2, 4)
        for i, d in enumerate((4, -4)):
            share(z, f_recv.at[i], d)
        for d in Z_DIRECT:
            share(z, v_recv, d)

    def gather_on(_):
        for i, (source, targets) in enumerate(((-4, (1, 2, 3, 4)), (4, (-1, -2, -3)))):
            wait_units(XBLOCK, f_recv.at[i])
            for d in targets:
                share(at_z(source), v_recv, d)

    def normalize(_):
        wait_units(13 * XBLOCK, v_recv)
        for b in range(NZ):
            nz[b] = xz[b].astype(jnp.float32) * as_column(iz[b], 16)

    def gain_local(_):
        for k in range(CH):
            cols = slice(CW * k, CW * (k + 1))
            acc = qz[k, 0] * nz[0, :, cols]
            for b in range(1, NZ):
                acc = acc + qz[k, b] * nz[b, :, cols]
            gown[:, cols] = jnp.sum(acc, axis=0, keepdims=True)
        grecv[z] = gown[...]
        pl.semaphore_wait(k_sem.at[2], 2)
        for j in range(1, NZ):
            copy_to(gown, grecv.at[z], g_recv, dev(z=at_z(j)))

    def gain_far(_):
        wait_bytes(grecv.at[pl.ds(0, NZ - 1)], g_recv)
        acc = grecv[0]
        for i in range(1, NZ):
            acc = acc + grecv[i]
        gsum[...] = acc
        gall[hi, mine] = acc
        for j in range(1, 2 * 16):
            copy_to(gsum, gall.at[hi, mine], a_recv, plane_peer(j))

    steps = {
        "gather": gather,
        "gather_on": gather_on,
        "normalize": normalize,
        "gain_local": gain_local,
        "gain_far": gain_far,
        "forward_x": forward_x,
        "forward_y": forward_y,
        "near": multiply_near,
        "far": multiply_far,
        "own": multiply_own,
        "add_y": add_y,
        "relay": relay,
        "add_z": add_z,
    }
    for step, k in SCHEDULE:
        with jax.named_scope(f"{step}_{k}"):
            steps[step](k)

    with jax.named_scope("send_rows"):
        rrow[mine] = trow[me]
        for j in range(1, 16):
            peer, _, theirs = group_peer(j)
            copy_to(trow.at[theirs], rrow.at[mine], t_recv, peer)

    with jax.named_scope("rows"):
        wait_bytes(rrow.at[pl.ds(0, 15)], t_recv)
        total = jnp.zeros((1, PW), jnp.float32)
        for j in range(PARTS):
            total = total + rrow[j] * gain[:, PW * j : PW * (j + 1)] * nown[j]
        inner = jnp.sum(total, axis=-1, keepdims=True) / D
        for j in range(PARTS):
            cols = slice(PW * j, PW * (j + 1))
            scaled = rrow[j] * gain[:, cols]
            out[:, cols] = (inv_rms * (scaled - nown[j] * inner)).astype(jnp.bfloat16)

    with jax.named_scope("gain_all"):
        wait_units(31 * PW * 4 // UNIT, a_recv)
        for j in range(PARTS):
            gout[:, PW * j : PW * (j + 1)] = gall[0, j] + gall[1, j]

    with jax.named_scope("drain"):
        wait_units(sum(sent), send_sem)


def per_device(inputs, norm_gain, gate_grad, up_grad, gate_weight, up_weight):
    f32, bf16 = jnp.float32, jnp.bfloat16
    dma = pltpu.SemaphoreType.DMA
    hbm = pl.BlockSpec(memory_space=pl.ANY)
    vmem = pl.BlockSpec(memory_space=pltpu.VMEM)
    input_grad, gain_grad = pl.pallas_call(
        kernel,
        out_shape=(jax.ShapeDtypeStruct((1, D), bf16), jax.ShapeDtypeStruct((1, D), f32)),
        in_specs=[hbm] * 6,
        out_specs=(vmem, vmem),
        scratch_shapes=[
            pltpu.VMEM((2, 128, 128), bf16),
            pltpu.VMEM((1, D), bf16),
            pltpu.VMEM((1, D), f32),
            pltpu.VMEM((NX, 2, 4, 64, 256), bf16),
            pltpu.VMEM((NX - 1, PW, 256), bf16),
            pltpu.VMEM((NX, PW, 256), bf16),
            pltpu.VMEM((CH, 2, 128, CW), bf16),
            pltpu.VMEM((CH, 2, 1, 128), f32),
            pltpu.VMEM((CH, 256, CW), f32),
            pltpu.VMEM((CH, 2, 128, CW), bf16),
            pltpu.VMEM((CH, 2, 1, 128), f32),
            pltpu.VMEM((CH, NZ, 16, CW), f32),
            pltpu.VMEM((CH, NZ, 16, CW), bf16),
            pltpu.VMEM((CH, NZ, 1, 128), f32),
            pltpu.VMEM((CH, 6, 16, CW), bf16),
            pltpu.VMEM((CH, 7, 16, CW), bf16),
            pltpu.VMEM((CH, 2, 16, CW), bf16),
            pltpu.VMEM((CH, 2, 16, CW), bf16),
            pltpu.VMEM((CH, 6, 1, 128), f32),
            pltpu.VMEM((CH, 7, 1, 128), f32),
            pltpu.VMEM((CH, 2, 1, 128), f32),
            pltpu.VMEM((CH, 2, 1, 128), f32),
            pltpu.VMEM((PARTS, 1, PW), f32),
            pltpu.VMEM((PARTS, 1, XW), f32),
            pltpu.VMEM((16, 1, XW), f32),
            pltpu.VMEM((16, XW), f32),
            pltpu.VMEM((NZ, 16, PW), bf16),
            pltpu.VMEM((NZ, 1, 128), f32),
            pltpu.VMEM((NZ, 16, PW), f32),
            pltpu.VMEM((16, 1, PW), f32),
            pltpu.VMEM((PARTS, 1, PW), f32),
            pltpu.VMEM((1, PW), f32),
            pltpu.VMEM((NZ, 1, PW), f32),
            pltpu.VMEM((1, PW), f32),
            pltpu.VMEM((2, PARTS, 1, PW), f32),
            pltpu.VMEM((6000, 1, 128), f32),
            pltpu.SemaphoreType.REGULAR((3,)),
            pltpu.SemaphoreType.REGULAR((2,)),
            dma((3,)),
            dma, dma,
            dma((3,)), dma((4,)), dma((2,)),
            dma((CH,)), dma((CH,)),
            dma((CH,)), dma((CH,)),
            dma, dma, dma((2,)),
            dma, dma, dma,
        ],
        compiler_params=pltpu.CompilerParams(collective_id=0, has_side_effects=True, vmem_limit_bytes=VMEM_GRANT),
    )(
        gate_weight,
        up_weight,
        gate_grad[0],
        up_grad[0],
        inputs[0],
        norm_gain.reshape(1, D),
    )
    def put(a, b, c, d, sem):
        copies = [pltpu.make_async_copy(a, c, sem.at[0]), pltpu.make_async_copy(b, d, sem.at[1])]
        for copy in copies:
            copy.start()
        for copy in copies:
            copy.wait()

    input_grad, gain_grad = pl.pallas_call(
        put,
        out_shape=(jax.ShapeDtypeStruct((1, D), bf16), jax.ShapeDtypeStruct((1, D), f32)),
        in_specs=[hbm, hbm],
        out_specs=(hbm, hbm),
        scratch_shapes=[dma((2,))],
        compiler_params=pltpu.CompilerParams(vmem_limit_bytes=2**20),
    )(input_grad, gain_grad)
    return (input_grad[None], gain_grad.reshape(D))


def solution(mesh):
    finer = Mesh(mesh.devices.reshape(2, 2, NZ, NX, 2), ("dp_0", "dp_1", "tp_0", "tp_1", "tp_2"))
    return jax.shard_map(
        per_device,
        mesh=finer,
        in_specs=(P(DP, TP, None), P(), P(DP, None, TP), P(DP, None, TP), P(None, TP), P(None, TP)),
        out_specs=(P(DP, TP, None), P()),
        check_vma=False,
    )
```

```python
import math

import jax
import jax.numpy as jnp
from jax import lax
from jax.experimental import pallas as pl
from jax.experimental.pallas import tpu as pltpu
from jax.sharding import Mesh
from jax.sharding import PartitionSpec as P

TP = ("tp_0", "tp_1", "tp_2")
DP = ("dp_0", "dp_1")
MESH = pl.DeviceIdType.MESH

epsilon = 1e-05

D = 8192
NX = 4
NZ = 16
PARTS = 16
PW = D // PARTS
CH = 4
CW = PW // CH
X_ORDER = (1, 3, 2)
VMEM_GRANT = 55150 * 1024
LEVELS = 240.0
UNIT = 512
BLOCK = 9
XBLOCK = 33
MIDDLE = 120.0
Z_DIRECT = (3, 2, 1, -3, -2, -1)
Z_UP, Z_DOWN = ((3, 7), (2, 6), (1, 5)), ((-3, -7), (-2, -6), (-1, -5))
Z_RELAY = (((4, 8),) + Z_UP + Z_DOWN, ((-4, -8),) + Z_DOWN + Z_UP)
XW = PW + 128
SCHEDULE = (
    ("forward_x", 1),
    ("forward_x", 3),
    ("forward_x", 2),
    ("forward_y", 0),
    ("forward_y", 1),
    ("gather", 0),
    ("forward_y", 3),
    ("near", 0),
    ("forward_y", 2),
    ("far", 0),
    ("own", 0),
    ("near", 1),
    ("far", 1),
    ("gather_on", 0),
    ("own", 1),
    ("add_y", 0),
    ("near", 2),
    ("far", 2),
    ("own", 2),
    ("near", 3),
    ("far", 3),
    ("own", 3),
    ("add_y", 1),
    ("add_y", 2),
    ("relay", 0),
    ("add_y", 3),
    ("normalize", 0),
    ("gain_local", 0),
    ("relay", 1),
    ("relay", 2),
    ("relay", 3),
    ("add_z", 0),
    ("add_z", 1),
    ("add_z", 2),
    ("gain_far", 0),
    ("add_z", 3),
)
NT = (((1,), (1,)), ((), ()))


def encode(v):
    size = jnp.abs(v)
    scale = jnp.maximum(jnp.max(size, axis=-1, keepdims=True) * 1.001, 1e-30)
    t = size * (LEVELS / scale)
    whole = jnp.floor(t)
    code = jnp.exp2(whole - MIDDLE) * (1.0 + (t - whole))
    return jnp.where(v < 0.0, -code, code).astype(jnp.bfloat16), scale


def decode(code, scale):
    code = code.astype(jnp.float32)
    size = jnp.abs(code)
    power = jnp.floor(jnp.log2(size))
    t = size * jnp.exp2(-power) + (power + (MIDDLE - 1.0))
    return jnp.where(code < 0.0, -t, t) * (scale * (1.0 / LEVELS))


def eye(rows):
    row = lax.broadcasted_iota(jnp.int32, (rows, 128), 0)
    lane = lax.broadcasted_iota(jnp.int32, (rows, 128), 1)
    return (row == lane).astype(jnp.float32)


def as_row(column):
    return jnp.sum(column * eye(column.shape[0]), axis=0, keepdims=True)


def as_column(row, rows):
    return jnp.sum(row * eye(rows), axis=-1, keepdims=True)


def wait_bytes(ref, sem):
    pltpu.make_async_copy(ref, ref, sem).wait()


def kernel(
    gw, uw, gg_in, ug_in, x_in, gain_in, out, gout,
    gug, xin, gain, cots, wst, wb, psend, spsend, pown, yr, syr, qz, qc, qs, rdir, rrel, srel, r2, srdir, srrel, ssrel, sr2, nown, xsend, nrecv, xf, xz, iz, nz, trow, rrow, gown, grecv, gsum, gall, units,
    k_sem, m_sem, in_sem, w_sem, send_sem, cx_recv, cy_recv, cc_recv, wx_recv, y_recv, zr_recv, zd_recv, n_recv, v_recv, f_recv,
    t_recv, g_recv, a_recv,
):
    lo, co = lax.axis_index("dp_0"), lax.axis_index("dp_1")
    z, x, hi = lax.axis_index("tp_0"), lax.axis_index("tp_1"), lax.axis_index("tp_2")

    def dev(lo=lo, co=co, z=z, x=x, hi=hi):
        return {"dp_0": lo, "dp_1": co, "tp_0": z, "tp_1": x, "tp_2": hi}

    def at_x(r):
        return lax.rem(x + r, NX)

    def at_z(d):
        return lax.rem(z + (d + NZ), NZ)

    side = lax.rem(lo + hi, 2)

    def part(x, side, co):
        return (x * 2 + side) * 2 + co

    def group_peer(j):
        dx, dlo, dco = j // 4, (j // 2) % 2, j % 2
        px, plo, pco = lax.rem(x + dx, NX), lax.rem(lo + dlo, 2), lax.rem(co + dco, 2)
        return dev(lo=plo, co=pco, x=px), part(px, lax.rem(plo + hi, 2), pco), (plo * 2 + pco) * NX + px

    def plane_peer(j):
        dx, dlo, dco, dhi = j // 8, (j // 4) % 2, (j // 2) % 2, j % 2
        return dev(lo=lax.rem(lo + dlo, 2), co=lax.rem(co + dco, 2), x=lax.rem(x + dx, NX), hi=lax.rem(hi + dhi, 2))

    def greet(step, d):
        for away in (d, -d):
            pl.semaphore_signal(k_sem.at[step], inc=1, device_id=dev(z=at_z(away)), device_id_type=MESH)

    mine = part(x, side, co)
    me = (lo * 2 + co) * NX + x
    seq = lo * 2 + co
    y_peer = dev(lo=1 - lo)
    core_peer = dev(co=1 - co)
    partner = dev(lo=1 - lo, hi=1 - hi)

    sent = []

    def copy_to(src, dst, recv, device):
        pltpu.make_async_remote_copy(
            src_ref=src, dst_ref=dst, send_sem=send_sem, recv_sem=recv, device_id=device, device_id_type=MESH
        ).start()
        sent.append(math.prod(src.shape) * src.dtype.itemsize // UNIT)

    def wait_units(count, sem):
        wait_bytes(units.at[pl.ds(0, count)], sem)

    loads = []
    pairs = ((gg_in, gug.at[0]), (ug_in, gug.at[1]), (x_in, xin), (gain_in, gain))
    for (src, dst), i in zip(pairs, (0, 0, 1, 2)):
        loads.append(pltpu.make_async_copy(src, dst, in_sem.at[i]))
        loads[-1].start()
    with jax.named_scope("signals"):
        barrier = pltpu.get_barrier_semaphore()
        near = [dev(x=at_x(r)) for r in X_ORDER] + [dev(z=at_z(1)), dev(z=at_z(-1)), y_peer, core_peer, partner]
        for peer in near:
            pl.semaphore_signal(barrier, inc=1, device_id=peer, device_id_type=MESH)

    for r in X_ORDER + (0,):
        rows = pl.ds(pl.multiple_of(part(at_x(r), side, co) * PW, PW), PW)
        target = wb.at[0] if r == 0 else wst.at[r - 1]
        for i, w in enumerate((gw, uw)):
            pltpu.make_async_copy(w.at[rows], target.at[:, pl.ds(128 * i, 128)], w_sem).start()

    with jax.named_scope("prepare"):
        to = lax.broadcasted_iota(jnp.int32, (128, 128), 0)
        token = lax.broadcasted_iota(jnp.int32, (128, 128), 1)
        order = (token == 2 * (to % 64) + to // 64).astype(jnp.float32).astype(jnp.bfloat16)
        wait_bytes(gug, in_sem.at[0])
        for i in range(2):
            ordered = jnp.dot(order, gug[i], preferred_element_type=jnp.float32).astype(jnp.bfloat16)
            for h in range(2):
                cots[0, h, seq, :, 128 * i : 128 * (i + 1)] = ordered[64 * h : 64 * (h + 1)]

    with jax.named_scope("barrier"):
        pl.semaphore_wait(barrier, len(near))

    def meet(step, *peers):
        for peer in peers:
            pl.semaphore_signal(m_sem.at[step], inc=1, device_id=peer, device_id_type=MESH)

    meet(0, y_peer, core_peer)
    greet(0, 1)

    with jax.named_scope("start_cots"):
        own = cots.at[0, :, seq]
        for r in X_ORDER:
            copy_to(own, cots.at[r, :, seq], cx_recv.at[r - 1], dev(x=at_x(r)))
        copy_to(own, own, cy_recv.at[0], y_peer)
        copy_to(own, own, cc_recv.at[0], core_peer)
        loads[2].wait()
        loads[3].wait()
        total = jnp.zeros((1, PW), jnp.float32)
        for j in range(PARTS):
            v = xin[:, PW * j : PW * (j + 1)].astype(jnp.float32)
            total = total + v * v
        inv_rms = lax.rsqrt(jnp.sum(total, axis=-1, keepdims=True) / D + epsilon)
        for j in range(PARTS):
            v = xin[:, PW * j : PW * (j + 1)].astype(jnp.float32)
            nown[j] = v * inv_rms
            xsend[j, :, :PW] = v
            xsend[j, :, PW:] = jnp.broadcast_to(inv_rms, (1, 128))
    with jax.named_scope("meet"):
        pl.semaphore_wait(m_sem.at[0], 2)
        meet(1, y_peer)
        pl.semaphore_wait(m_sem.at[1], 1)
        pl.semaphore_wait(k_sem.at[0], 2)
        greet(1, 2)
    with jax.named_scope("start_sends"):
        nrecv[me] = xsend[mine]
        for j in range(1, 16):
            peer, theirs, _ = group_peer(j)
            copy_to(xsend.at[theirs], nrecv.at[me], n_recv, peer)
        wait_bytes(wb, w_sem)
        for k in range(CH):
            rows = pl.ds(CW * k, CW)
            for r in X_ORDER:
                copy_to(wst.at[r - 1, rows], wb.at[r, rows], wx_recv.at[k], dev(x=at_x(r)))

    other = (1 - lo) * 2 + co

    def forward_x(r):
        block = cots.at[r, :, seq]
        wait_bytes(block, cx_recv.at[r - 1])
        copy_to(block, block, cy_recv.at[r], y_peer)
        copy_to(block, block, cc_recv.at[0], core_peer)

    def forward_y(r):
        block = cots.at[r, :, other]
        wait_bytes(block, cy_recv.at[r])
        copy_to(block, block, cc_recv.at[1], core_peer)

    def product(block, k):
        acc = 0.0
        for r in range(NX):
            rows = block(r)
            rows = rows.reshape(rows.shape[0] * 64, 256)
            acc = acc + lax.dot_general(rows, wb[r, CW * k : CW * (k + 1)], NT, preferred_element_type=jnp.float32)
        return acc

    def multiply(l, b, k):
        if k == 0:
            wait_bytes(cots.at[:, :, 0], cc_recv.at[b])
        if b == 0:
            wait_bytes(wb.at[pl.ds(0, 3), pl.ds(0, CW)], wx_recv.at[k])
        code, scale = encode(product(lambda r: cots[r, 1 - hi, pl.ds(2 * l, 2)], k))
        psend[k, l] = code
        spsend[k, l] = as_row(scale)
        copy_to(psend.at[k, l], yr.at[k, l], y_recv.at[k], partner)
        copy_to(spsend.at[k, l], syr.at[k, l], y_recv.at[k], partner)

    def multiply_near(k):
        multiply(lo, 0, k)

    def multiply_far(k):
        multiply(1 - lo, 1, k)

    def multiply_own(k):
        pown[k] = product(lambda r: cots[r, hi], k)

    def add_y(k):
        wait_units(2 * (64 + 1), y_recv.at[k])
        for l in range(2):
            scale = as_column(syr[k, l], 128)
            half = slice(128 * l, 128 * (l + 1))
            pown[k, half] = pown[k, half] + decode(yr[k, l], scale)
        for b in range(NZ):
            for s in range(4):
                rows = slice(s * 64 + b * 4, s * 64 + b * 4 + 4)
                qz[k, b, 4 * s : 4 * s + 4] = pown[k, rows]
        code, scale = encode(qz[k])
        qc[k] = code
        qs[k] = jnp.sum(scale * eye(16), axis=1, keepdims=True)
        for i, (d, far) in enumerate(Z_RELAY[k % 2]):
            copy_to(qc.at[k, at_z(far)], rrel.at[k, i], zr_recv.at[k], dev(z=at_z(d)))
            copy_to(qs.at[k, at_z(far)], srrel.at[k, i], zr_recv.at[k], dev(z=at_z(d)))
        for i, d in enumerate(Z_DIRECT):
            copy_to(qc.at[k, at_z(d)], rdir.at[k, i], zd_recv.at[k], dev(z=at_z(d)))
            copy_to(qs.at[k, at_z(d)], srdir.at[k, i], zd_recv.at[k], dev(z=at_z(d)))

    def relay(k):
        wait_units(7 * BLOCK, zr_recv.at[k])
        first = 4 if k % 2 == 0 else -4
        for i, (d, sources) in enumerate(((first, (0, 1, 2, 3)), (-first, (4, 5, 6)))):
            acc = qz[k, at_z(d)]
            for j in sources:
                acc = acc + decode(rrel[k, j], as_column(srrel[k, j], 16))
            code, scale = encode(acc)
            srel[k, i] = code
            ssrel[k, i] = as_row(scale)
            copy_to(srel.at[k, i], r2.at[k, i], zd_recv.at[k], dev(z=at_z(d)))
            copy_to(ssrel.at[k, i], sr2.at[k, i], zd_recv.at[k], dev(z=at_z(d)))

    def add_z(k):
        wait_units(8 * BLOCK, zd_recv.at[k])
        acc = qz[k, z]
        for i in range(6):
            acc = acc + decode(rdir[k, i], as_column(srdir[k, i], 16))
        for i in range(2):
            acc = acc + decode(r2[k, i], as_column(sr2[k, i], 16))
        for i in range(16):
            trow[i, :, CW * k : CW * (k + 1)] = acc[i : i + 1]

    def share(b, sem, d):
        for ref in (xz, iz):
            copy_to(ref.at[b], ref.at[b], sem, dev(z=at_z(d)))

    def gather(_):
        wait_bytes(nrecv.at[pl.ds(0, 15)], n_recv)
        for i in range(16):
            xf[i : i + 1] = nrecv[i]
        xz[z] = xf[:, :PW].astype(jnp.bfloat16)
        iz[z] = as_row(xf[:, PW : PW + 1])
        pl.semaphore_wait(k_sem.at[1], 2)
        greet(2, 4)
        for i, d in enumerate((4, -4)):
            share(z, f_recv.at[i], d)
        for d in Z_DIRECT:
            share(z, v_recv, d)

    def gather_on(_):
        for i, (source, targets) in enumerate(((-4, (1, 2, 3, 4)), (4, (-1, -2, -3)))):
            wait_units(XBLOCK, f_recv.at[i])
            for d in targets:
                share(at_z(source), v_recv, d)

    def normalize(_):
        wait_units(13 * XBLOCK, v_recv)
        for b in range(NZ):
            nz[b] = xz[b].astype(jnp.float32) * as_column(iz[b], 16)

    def gain_local(_):
        for k in range(CH):
            cols = slice(CW * k, CW * (k + 1))
            acc = qz[k, 0] * nz[0, :, cols]
            for b in range(1, NZ):
                acc = acc + qz[k, b] * nz[b, :, cols]
            gown[:, cols] = jnp.sum(acc, axis=0, keepdims=True)
        grecv[z] = gown[...]
        pl.semaphore_wait(k_sem.at[2], 2)
        for j in range(1, NZ):
            copy_to(gown, grecv.at[z], g_recv, dev(z=at_z(j)))

    def gain_far(_):
        wait_bytes(grecv.at[pl.ds(0, NZ - 1)], g_recv)
        acc = grecv[0]
        for i in range(1, NZ):
            acc = acc + grecv[i]
        gsum[...] = acc
        gall[hi, mine] = acc
        for j in range(1, 2 * 16):
            copy_to(gsum, gall.at[hi, mine], a_recv, plane_peer(j))

    steps = {
        "gather": gather,
        "gather_on": gather_on,
        "normalize": normalize,
        "gain_local": gain_local,
        "gain_far": gain_far,
        "forward_x": forward_x,
        "forward_y": forward_y,
        "near": multiply_near,
        "far": multiply_far,
        "own": multiply_own,
        "add_y": add_y,
        "relay": relay,
        "add_z": add_z,
    }
    for step, k in SCHEDULE:
        with jax.named_scope(f"{step}_{k}"):
            steps[step](k)

    with jax.named_scope("send_rows"):
        rrow[mine] = trow[me]
        for j in range(1, 16):
            peer, _, theirs = group_peer(j)
            copy_to(trow.at[theirs], rrow.at[mine], t_recv, peer)

    with jax.named_scope("rows"):
        wait_bytes(rrow.at[pl.ds(0, 15)], t_recv)
        total = jnp.zeros((1, PW), jnp.float32)
        for j in range(PARTS):
            total = total + rrow[j] * gain[:, PW * j : PW * (j + 1)] * nown[j]
        inner = jnp.sum(total, axis=-1, keepdims=True) / D
        for j in range(PARTS):
            cols = slice(PW * j, PW * (j + 1))
            scaled = rrow[j] * gain[:, cols]
            out[:, cols] = (inv_rms * (scaled - nown[j] * inner)).astype(jnp.bfloat16)

    with jax.named_scope("gain_all"):
        wait_units(31 * PW * 4 // UNIT, a_recv)
        for j in range(PARTS):
            gout[:, PW * j : PW * (j + 1)] = gall[0, j] + gall[1, j]

    with jax.named_scope("drain"):
        wait_units(sum(sent), send_sem)


def per_device(inputs, norm_gain, gate_grad, up_grad, gate_weight, up_weight):
    f32, bf16 = jnp.float32, jnp.bfloat16
    dma = pltpu.SemaphoreType.DMA
    hbm = pl.BlockSpec(memory_space=pl.ANY)
    vmem = pl.BlockSpec(memory_space=pltpu.VMEM)
    input_grad, gain_grad = pl.pallas_call(
        kernel,
        out_shape=(jax.ShapeDtypeStruct((1, D), bf16), jax.ShapeDtypeStruct((1, D), f32)),
        in_specs=[hbm] * 6,
        out_specs=(vmem, vmem),
        scratch_shapes=[
            pltpu.VMEM((2, 128, 128), bf16),
            pltpu.VMEM((1, D), bf16),
            pltpu.VMEM((1, D), f32),
            pltpu.VMEM((NX, 2, 4, 64, 256), bf16),
            pltpu.VMEM((NX - 1, PW, 256), bf16),
            pltpu.VMEM((NX, PW, 256), bf16),
            pltpu.VMEM((CH, 2, 128, CW), bf16),
            pltpu.VMEM((CH, 2, 1, 128), f32),
            pltpu.VMEM((CH, 256, CW), f32),
            pltpu.VMEM((CH, 2, 128, CW), bf16),
            pltpu.VMEM((CH, 2, 1, 128), f32),
            pltpu.VMEM((CH, NZ, 16, CW), f32),
            pltpu.VMEM((CH, NZ, 16, CW), bf16),
            pltpu.VMEM((CH, NZ, 1, 128), f32),
            pltpu.VMEM((CH, 6, 16, CW), bf16),
            pltpu.VMEM((CH, 7, 16, CW), bf16),
            pltpu.VMEM((CH, 2, 16, CW), bf16),
            pltpu.VMEM((CH, 2, 16, CW), bf16),
            pltpu.VMEM((CH, 6, 1, 128), f32),
            pltpu.VMEM((CH, 7, 1, 128), f32),
            pltpu.VMEM((CH, 2, 1, 128), f32),
            pltpu.VMEM((CH, 2, 1, 128), f32),
            pltpu.VMEM((PARTS, 1, PW), f32),
            pltpu.VMEM((PARTS, 1, XW), f32),
            pltpu.VMEM((16, 1, XW), f32),
            pltpu.VMEM((16, XW), f32),
            pltpu.VMEM((NZ, 16, PW), bf16),
            pltpu.VMEM((NZ, 1, 128), f32),
            pltpu.VMEM((NZ, 16, PW), f32),
            pltpu.VMEM((16, 1, PW), f32),
            pltpu.VMEM((PARTS, 1, PW), f32),
            pltpu.VMEM((1, PW), f32),
            pltpu.VMEM((NZ, 1, PW), f32),
            pltpu.VMEM((1, PW), f32),
            pltpu.VMEM((2, PARTS, 1, PW), f32),
            pltpu.VMEM((6000, 1, 128), f32),
            pltpu.SemaphoreType.REGULAR((3,)),
            pltpu.SemaphoreType.REGULAR((2,)),
            dma((3,)),
            dma, dma,
            dma((3,)), dma((4,)), dma((2,)),
            dma((CH,)), dma((CH,)),
            dma((CH,)), dma((CH,)),
            dma, dma, dma((2,)),
            dma, dma, dma,
        ],
        compiler_params=pltpu.CompilerParams(collective_id=0, has_side_effects=True, vmem_limit_bytes=VMEM_GRANT),
    )(
        gate_weight,
        up_weight,
        gate_grad[0],
        up_grad[0],
        inputs[0],
        norm_gain.reshape(1, D),
    )
    def put(a, b, c, d, sem):
        copies = [pltpu.make_async_copy(a, c, sem.at[0]), pltpu.make_async_copy(b, d, sem.at[1])]
        for copy in copies:
            copy.start()
        for copy in copies:
            copy.wait()

    input_grad, gain_grad = pl.pallas_call(
        put,
        out_shape=(jax.ShapeDtypeStruct((1, D), bf16), jax.ShapeDtypeStruct((1, D), f32)),
        in_specs=[hbm, hbm],
        out_specs=(hbm, hbm),
        scratch_shapes=[dma((2,))],
        compiler_params=pltpu.CompilerParams(vmem_limit_bytes=2**20),
    )(input_grad, gain_grad)
    return (input_grad[None], gain_grad.reshape(D))


def solution(mesh):
    finer = Mesh(mesh.devices.reshape(2, 2, NZ, NX, 2), ("dp_0", "dp_1", "tp_0", "tp_1", "tp_2"))
    return jax.shard_map(
        per_device,
        mesh=finer,
        in_specs=(P(DP, TP, None), P(), P(DP, None, TP), P(DP, None, TP), P(None, TP), P(None, TP)),
        out_specs=(P(DP, TP, None), P()),
        check_vma=False,
    )
```

```python
import math

import jax
import jax.numpy as jnp
from jax import lax
from jax.experimental import pallas as pl
from jax.experimental.pallas import tpu as pltpu
from jax.sharding import Mesh
from jax.sharding import PartitionSpec as P

TP = ("tp_0", "tp_1", "tp_2")
DP = ("dp_0", "dp_1")
MESH = pl.DeviceIdType.MESH

epsilon = 1e-05

D = 8192
NX = 4
NZ = 16
PARTS = 16
PW = D // PARTS
CH = 4
CW = PW // CH
X_ORDER = (2, 1, 3)
VMEM_GRANT = 55150 * 1024
LEVELS = 240.0
UNIT = 512
BLOCK = 9
XBLOCK = 33
MIDDLE = 120.0
Z_FAR_FIRST = (8, 7, 9, 6, 10, 5, 11, 4, 12, 3, 13, 2, 14, 1, 15)
Z_DIRECT = (3, 2, 1, -3, -2, -1)
Z_UP, Z_DOWN = ((3, 7), (2, 6), (1, 5)), ((-3, -7), (-2, -6), (-1, -5))
Z_RELAY = (((4, 8),) + Z_UP + Z_DOWN, ((-4, -8),) + Z_DOWN + Z_UP)
XW = PW + 128
SCHEDULE = (
    ("forward_x", 1),
    ("forward_x", 3),
    ("forward_x", 2),
    ("forward_y", 0),
    ("forward_y", 1),
    ("gather", 0),
    ("forward_y", 3),
    ("near", 0),
    ("forward_y", 2),
    ("far", 0),
    ("own", 0),
    ("near", 1),
    ("far", 1),
    ("gather_on", 0),
    ("own", 1),
    ("add_y", 0),
    ("near", 2),
    ("far", 2),
    ("own", 2),
    ("near", 3),
    ("far", 3),
    ("own", 3),
    ("add_y", 1),
    ("add_y", 2),
    ("relay", 0),
    ("add_y", 3),
    ("normalize", 0),
    ("gain_local", 0),
    ("relay", 1),
    ("relay", 2),
    ("relay", 3),
    ("add_z", 0),
    ("add_z", 1),
    ("add_z", 2),
    ("gain_far", 0),
    ("add_z", 3),
)
NT = (((1,), (1,)), ((), ()))


def encode(v):
    size = jnp.abs(v)
    scale = jnp.maximum(jnp.max(size, axis=-1, keepdims=True) * 1.001, 1e-30)
    t = size * (LEVELS / scale)
    whole = jnp.floor(t)
    code = jnp.exp2(whole - MIDDLE) * (1.0 + (t - whole))
    return jnp.where(v < 0.0, -code, code).astype(jnp.bfloat16), scale


def decode(code, scale):
    code = code.astype(jnp.float32)
    size = jnp.abs(code)
    power = jnp.floor(jnp.log2(size))
    t = size * jnp.exp2(-power) + (power + (MIDDLE - 1.0))
    return jnp.where(code < 0.0, -t, t) * (scale * (1.0 / LEVELS))


def eye(rows):
    row = lax.broadcasted_iota(jnp.int32, (rows, 128), 0)
    lane = lax.broadcasted_iota(jnp.int32, (rows, 128), 1)
    return (row == lane).astype(jnp.float32)


def as_row(column):
    return jnp.sum(column * eye(column.shape[0]), axis=0, keepdims=True)


def as_column(row, rows):
    return jnp.sum(row * eye(rows), axis=-1, keepdims=True)


def wait_bytes(ref, sem):
    pltpu.make_async_copy(ref, ref, sem).wait()


def kernel(
    gw, uw, gg_in, ug_in, x_in, gain_in, out, gout,
    gug, xin, gain, cots, wst, wb, psend, spsend, pown, yr, syr, qz, qc, qs, rdir, rrel, srel, r2, srdir, srrel, ssrel, sr2, nown, xsend, nrecv, xf, xz, iz, nz, trow, rrow, gown, grecv, gsum, gall, units,
    k_sem, m_sem, in_sem, w_sem, send_sem, cx_recv, cy_recv, cc_recv, wx_recv, y_recv, zr_recv, zd_recv, n_recv, v_recv, f_recv,
    t_recv, g_recv, a_recv,
):
    lo, co = lax.axis_index("dp_0"), lax.axis_index("dp_1")
    z, x, hi = lax.axis_index("tp_0"), lax.axis_index("tp_1"), lax.axis_index("tp_2")

    def dev(lo=lo, co=co, z=z, x=x, hi=hi):
        return {"dp_0": lo, "dp_1": co, "tp_0": z, "tp_1": x, "tp_2": hi}

    def at_x(r):
        return lax.rem(x + r, NX)

    def at_z(d):
        return lax.rem(z + (d + NZ), NZ)

    side = lax.rem(lo + hi, 2)

    def part(x, side, co):
        return (x * 2 + side) * 2 + co

    def group_peer(j):
        dx, dlo, dco = j // 4, (j // 2) % 2, j % 2
        px, plo, pco = lax.rem(x + dx, NX), lax.rem(lo + dlo, 2), lax.rem(co + dco, 2)
        return dev(lo=plo, co=pco, x=px), part(px, lax.rem(plo + hi, 2), pco), (plo * 2 + pco) * NX + px

    def plane_peer(j):
        dx, dlo, dco, dhi = j // 8, (j // 4) % 2, (j // 2) % 2, j % 2
        return dev(lo=lax.rem(lo + dlo, 2), co=lax.rem(co + dco, 2), x=lax.rem(x + dx, NX), hi=lax.rem(hi + dhi, 2))

    def greet(step, d):
        for away in (d, -d):
            pl.semaphore_signal(k_sem.at[step], inc=1, device_id=dev(z=at_z(away)), device_id_type=MESH)

    mine = part(x, side, co)
    me = (lo * 2 + co) * NX + x
    seq = lo * 2 + co
    y_peer = dev(lo=1 - lo)
    core_peer = dev(co=1 - co)
    partner = dev(lo=1 - lo, hi=1 - hi)

    sent = []

    def copy_to(src, dst, recv, device):
        pltpu.make_async_remote_copy(
            src_ref=src, dst_ref=dst, send_sem=send_sem, recv_sem=recv, device_id=device, device_id_type=MESH
        ).start()
        sent.append(math.prod(src.shape) * src.dtype.itemsize // UNIT)

    def wait_units(count, sem):
        wait_bytes(units.at[pl.ds(0, count)], sem)

    loads = []
    pairs = ((gg_in, gug.at[0]), (ug_in, gug.at[1]), (x_in, xin), (gain_in, gain))
    for (src, dst), i in zip(pairs, (0, 0, 1, 2)):
        loads.append(pltpu.make_async_copy(src, dst, in_sem.at[i]))
        loads[-1].start()
    with jax.named_scope("signals"):
        barrier = pltpu.get_barrier_semaphore()
        near = [dev(x=at_x(r)) for r in X_ORDER] + [dev(z=at_z(1)), dev(z=at_z(-1)), y_peer, core_peer, partner]
        for peer in near:
            pl.semaphore_signal(barrier, inc=1, device_id=peer, device_id_type=MESH)

    for r in X_ORDER + (0,):
        rows = pl.ds(pl.multiple_of(part(at_x(r), side, co) * PW, PW), PW)
        target = wb.at[0] if r == 0 else wst.at[r - 1]
        for i, w in enumerate((gw, uw)):
            pltpu.make_async_copy(w.at[rows], target.at[:, pl.ds(128 * i, 128)], w_sem).start()

    with jax.named_scope("prepare"):
        to = lax.broadcasted_iota(jnp.int32, (128, 128), 0)
        token = lax.broadcasted_iota(jnp.int32, (128, 128), 1)
        order = (token == 2 * (to % 64) + to // 64).astype(jnp.float32).astype(jnp.bfloat16)
        wait_bytes(gug, in_sem.at[0])
        for i in range(2):
            ordered = jnp.dot(order, gug[i], preferred_element_type=jnp.float32).astype(jnp.bfloat16)
            for h in range(2):
                cots[0, h, seq, :, 128 * i : 128 * (i + 1)] = ordered[64 * h : 64 * (h + 1)]

    with jax.named_scope("barrier"):
        pl.semaphore_wait(barrier, len(near))

    def meet(step, *peers):
        for peer in peers:
            pl.semaphore_signal(m_sem.at[step], inc=1, device_id=peer, device_id_type=MESH)

    meet(0, y_peer, core_peer)
    greet(0, 1)

    with jax.named_scope("start_cots"):
        own = cots.at[0, :, seq]
        for r in X_ORDER:
            copy_to(own, cots.at[r, :, seq], cx_recv.at[r - 1], dev(x=at_x(r)))
        copy_to(own, own, cy_recv.at[0], y_peer)
        copy_to(own, own, cc_recv.at[0], core_peer)
        loads[2].wait()
        loads[3].wait()
        total = jnp.zeros((1, PW), jnp.float32)
        for j in range(PARTS):
            v = xin[:, PW * j : PW * (j + 1)].astype(jnp.float32)
            total = total + v * v
        inv_rms = lax.rsqrt(jnp.sum(total, axis=-1, keepdims=True) / D + epsilon)
        for j in range(PARTS):
            v = xin[:, PW * j : PW * (j + 1)].astype(jnp.float32)
            nown[j] = v * inv_rms
            xsend[j, :, :PW] = v
            xsend[j, :, PW:] = jnp.broadcast_to(inv_rms, (1, 128))
    with jax.named_scope("meet"):
        pl.semaphore_wait(m_sem.at[0], 2)
        meet(1, y_peer)
        pl.semaphore_wait(m_sem.at[1], 1)
        pl.semaphore_wait(k_sem.at[0], 2)
        greet(1, 2)
    with jax.named_scope("start_sends"):
        nrecv[me] = xsend[mine]
        for j in range(1, 16):
            peer, theirs, _ = group_peer(j)
            copy_to(xsend.at[theirs], nrecv.at[me], n_recv, peer)
        wait_bytes(wb, w_sem)
        for k in range(CH):
            rows = pl.ds(CW * k, CW)
            for r in X_ORDER:
                copy_to(wst.at[r - 1, rows], wb.at[r, rows], wx_recv.at[k], dev(x=at_x(r)))

    other = (1 - lo) * 2 + co

    def forward_x(r):
        block = cots.at[r, :, seq]
        wait_bytes(block, cx_recv.at[r - 1])
        copy_to(block, block, cy_recv.at[r], y_peer)
        copy_to(block, block, cc_recv.at[0], core_peer)

    def forward_y(r):
        block = cots.at[r, :, other]
        wait_bytes(block, cy_recv.at[r])
        copy_to(block, block, cc_recv.at[1], core_peer)

    def product(block, k):
        acc = 0.0
        for r in range(NX):
            rows = block(r)
            rows = rows.reshape(rows.shape[0] * 64, 256)
            acc = acc + lax.dot_general(rows, wb[r, CW * k : CW * (k + 1)], NT, preferred_element_type=jnp.float32)
        return acc

    def multiply(l, b, k):
        if k == 0:
            wait_bytes(cots.at[:, :, 0], cc_recv.at[b])
        if b == 0:
            wait_bytes(wb.at[pl.ds(0, 3), pl.ds(0, CW)], wx_recv.at[k])
        code, scale = encode(product(lambda r: cots[r, 1 - hi, pl.ds(2 * l, 2)], k))
        psend[k, l] = code
        spsend[k, l] = as_row(scale)
        copy_to(psend.at[k, l], yr.at[k, l], y_recv.at[k], partner)
        copy_to(spsend.at[k, l], syr.at[k, l], y_recv.at[k], partner)

    def multiply_near(k):
        multiply(lo, 0, k)

    def multiply_far(k):
        multiply(1 - lo, 1, k)

    def multiply_own(k):
        pown[k] = product(lambda r: cots[r, hi], k)

    def add_y(k):
        wait_units(2 * (64 + 1), y_recv.at[k])
        for l in range(2):
            scale = as_column(syr[k, l], 128)
            half = slice(128 * l, 128 * (l + 1))
            pown[k, half] = pown[k, half] + decode(yr[k, l], scale)
        for b in range(NZ):
            for s in range(4):
                rows = slice(s * 64 + b * 4, s * 64 + b * 4 + 4)
                qz[k, b, 4 * s : 4 * s + 4] = pown[k, rows]
        code, scale = encode(qz[k])
        qc[k] = code
        qs[k] = jnp.sum(scale * eye(16), axis=1, keepdims=True)
        for i, (d, far) in enumerate(Z_RELAY[k % 2]):
            copy_to(qc.at[k, at_z(far)], rrel.at[k, i], zr_recv.at[k], dev(z=at_z(d)))
            copy_to(qs.at[k, at_z(far)], srrel.at[k, i], zr_recv.at[k], dev(z=at_z(d)))
        for i, d in enumerate(Z_DIRECT):
            copy_to(qc.at[k, at_z(d)], rdir.at[k, i], zd_recv.at[k], dev(z=at_z(d)))
            copy_to(qs.at[k, at_z(d)], srdir.at[k, i], zd_recv.at[k], dev(z=at_z(d)))

    def relay(k):
        wait_units(7 * BLOCK, zr_recv.at[k])
        first = 4 if k % 2 == 0 else -4
        for i, (d, sources) in enumerate(((first, (0, 1, 2, 3)), (-first, (4, 5, 6)))):
            acc = qz[k, at_z(d)]
            for j in sources:
                acc = acc + decode(rrel[k, j], as_column(srrel[k, j], 16))
            code, scale = encode(acc)
            srel[k, i] = code
            ssrel[k, i] = as_row(scale)
            copy_to(srel.at[k, i], r2.at[k, i], zd_recv.at[k], dev(z=at_z(d)))
            copy_to(ssrel.at[k, i], sr2.at[k, i], zd_recv.at[k], dev(z=at_z(d)))

    def add_z(k):
        wait_units(8 * BLOCK, zd_recv.at[k])
        acc = qz[k, z]
        for i in range(6):
            acc = acc + decode(rdir[k, i], as_column(srdir[k, i], 16))
        for i in range(2):
            acc = acc + decode(r2[k, i], as_column(sr2[k, i], 16))
        for i in range(16):
            trow[i, :, CW * k : CW * (k + 1)] = acc[i : i + 1]

    def share(b, sem, d):
        for ref in (xz, iz):
            copy_to(ref.at[b], ref.at[b], sem, dev(z=at_z(d)))

    def gather(_):
        wait_bytes(nrecv.at[pl.ds(0, 15)], n_recv)
        for i in range(16):
            xf[i : i + 1] = nrecv[i]
        xz[z] = xf[:, :PW].astype(jnp.bfloat16)
        iz[z] = as_row(xf[:, PW : PW + 1])
        pl.semaphore_wait(k_sem.at[1], 2)
        greet(2, 4)
        for i, d in enumerate((4, -4)):
            share(z, f_recv.at[i], d)
        for d in Z_DIRECT:
            share(z, v_recv, d)

    def gather_on(_):
        for i, (source, targets) in enumerate(((-4, (1, 2, 3, 4)), (4, (-1, -2, -3)))):
            wait_units(XBLOCK, f_recv.at[i])
            for d in targets:
                share(at_z(source), v_recv, d)

    def normalize(_):
        wait_units(13 * XBLOCK, v_recv)
        for b in range(NZ):
            nz[b] = xz[b].astype(jnp.float32) * as_column(iz[b], 16)

    def gain_local(_):
        for k in range(CH):
            cols = slice(CW * k, CW * (k + 1))
            acc = qz[k, 0] * nz[0, :, cols]
            for b in range(1, NZ):
                acc = acc + qz[k, b] * nz[b, :, cols]
            gown[:, cols] = jnp.sum(acc, axis=0, keepdims=True)
        grecv[z] = gown[...]
        pl.semaphore_wait(k_sem.at[2], 2)
        for j in Z_FAR_FIRST:
            copy_to(gown, grecv.at[z], g_recv, dev(z=at_z(j)))

    def gain_far(_):
        wait_bytes(grecv.at[pl.ds(0, NZ - 1)], g_recv)
        acc = grecv[0]
        for i in range(1, NZ):
            acc = acc + grecv[i]
        gsum[...] = acc
        gall[hi, mine] = acc
        for j in range(1, 2 * 16):
            copy_to(gsum, gall.at[hi, mine], a_recv, plane_peer(j))

    steps = {
        "gather": gather,
        "gather_on": gather_on,
        "normalize": normalize,
        "gain_local": gain_local,
        "gain_far": gain_far,
        "forward_x": forward_x,
        "forward_y": forward_y,
        "near": multiply_near,
        "far": multiply_far,
        "own": multiply_own,
        "add_y": add_y,
        "relay": relay,
        "add_z": add_z,
    }
    for step, k in SCHEDULE:
        with jax.named_scope(f"{step}_{k}"):
            steps[step](k)

    with jax.named_scope("send_rows"):
        rrow[mine] = trow[me]
        for j in range(1, 16):
            peer, _, theirs = group_peer(j)
            copy_to(trow.at[theirs], rrow.at[mine], t_recv, peer)

    with jax.named_scope("rows"):
        wait_bytes(rrow.at[pl.ds(0, 15)], t_recv)
        total = jnp.zeros((1, PW), jnp.float32)
        for j in range(PARTS):
            total = total + rrow[j] * gain[:, PW * j : PW * (j + 1)] * nown[j]
        inner = jnp.sum(total, axis=-1, keepdims=True) / D
        for j in range(PARTS):
            cols = slice(PW * j, PW * (j + 1))
            scaled = rrow[j] * gain[:, cols]
            out[:, cols] = (inv_rms * (scaled - nown[j] * inner)).astype(jnp.bfloat16)

    with jax.named_scope("gain_all"):
        wait_units(31 * PW * 4 // UNIT, a_recv)
        for j in range(PARTS):
            gout[:, PW * j : PW * (j + 1)] = gall[0, j] + gall[1, j]

    with jax.named_scope("drain"):
        wait_units(sum(sent), send_sem)


def per_device(inputs, norm_gain, gate_grad, up_grad, gate_weight, up_weight):
    f32, bf16 = jnp.float32, jnp.bfloat16
    dma = pltpu.SemaphoreType.DMA
    hbm = pl.BlockSpec(memory_space=pl.ANY)
    vmem = pl.BlockSpec(memory_space=pltpu.VMEM)
    input_grad, gain_grad = pl.pallas_call(
        kernel,
        out_shape=(jax.ShapeDtypeStruct((1, D), bf16), jax.ShapeDtypeStruct((1, D), f32)),
        in_specs=[hbm] * 6,
        out_specs=(vmem, vmem),
        scratch_shapes=[
            pltpu.VMEM((2, 128, 128), bf16),
            pltpu.VMEM((1, D), bf16),
            pltpu.VMEM((1, D), f32),
            pltpu.VMEM((NX, 2, 4, 64, 256), bf16),
            pltpu.VMEM((NX - 1, PW, 256), bf16),
            pltpu.VMEM((NX, PW, 256), bf16),
            pltpu.VMEM((CH, 2, 128, CW), bf16),
            pltpu.VMEM((CH, 2, 1, 128), f32),
            pltpu.VMEM((CH, 256, CW), f32),
            pltpu.VMEM((CH, 2, 128, CW), bf16),
            pltpu.VMEM((CH, 2, 1, 128), f32),
            pltpu.VMEM((CH, NZ, 16, CW), f32),
            pltpu.VMEM((CH, NZ, 16, CW), bf16),
            pltpu.VMEM((CH, NZ, 1, 128), f32),
            pltpu.VMEM((CH, 6, 16, CW), bf16),
            pltpu.VMEM((CH, 7, 16, CW), bf16),
            pltpu.VMEM((CH, 2, 16, CW), bf16),
            pltpu.VMEM((CH, 2, 16, CW), bf16),
            pltpu.VMEM((CH, 6, 1, 128), f32),
            pltpu.VMEM((CH, 7, 1, 128), f32),
            pltpu.VMEM((CH, 2, 1, 128), f32),
            pltpu.VMEM((CH, 2, 1, 128), f32),
            pltpu.VMEM((PARTS, 1, PW), f32),
            pltpu.VMEM((PARTS, 1, XW), f32),
            pltpu.VMEM((16, 1, XW), f32),
            pltpu.VMEM((16, XW), f32),
            pltpu.VMEM((NZ, 16, PW), bf16),
            pltpu.VMEM((NZ, 1, 128), f32),
            pltpu.VMEM((NZ, 16, PW), f32),
            pltpu.VMEM((16, 1, PW), f32),
            pltpu.VMEM((PARTS, 1, PW), f32),
            pltpu.VMEM((1, PW), f32),
            pltpu.VMEM((NZ, 1, PW), f32),
            pltpu.VMEM((1, PW), f32),
            pltpu.VMEM((2, PARTS, 1, PW), f32),
            pltpu.VMEM((6000, 1, 128), f32),
            pltpu.SemaphoreType.REGULAR((3,)),
            pltpu.SemaphoreType.REGULAR((2,)),
            dma((3,)),
            dma, dma,
            dma((3,)), dma((4,)), dma((2,)),
            dma((CH,)), dma((CH,)),
            dma((CH,)), dma((CH,)),
            dma, dma, dma((2,)),
            dma, dma, dma,
        ],
        compiler_params=pltpu.CompilerParams(collective_id=0, has_side_effects=True, vmem_limit_bytes=VMEM_GRANT),
    )(
        gate_weight,
        up_weight,
        gate_grad[0],
        up_grad[0],
        inputs[0],
        norm_gain.reshape(1, D),
    )
    def put(a, b, c, d, sem):
        copies = [pltpu.make_async_copy(a, c, sem.at[0]), pltpu.make_async_copy(b, d, sem.at[1])]
        for copy in copies:
            copy.start()
        for copy in copies:
            copy.wait()

    input_grad, gain_grad = pl.pallas_call(
        put,
        out_shape=(jax.ShapeDtypeStruct((1, D), bf16), jax.ShapeDtypeStruct((1, D), f32)),
        in_specs=[hbm, hbm],
        out_specs=(hbm, hbm),
        scratch_shapes=[dma((2,))],
        compiler_params=pltpu.CompilerParams(vmem_limit_bytes=2**20),
    )(input_grad, gain_grad)
    return (input_grad[None], gain_grad.reshape(D))


def solution(mesh):
    finer = Mesh(mesh.devices.reshape(2, 2, NZ, NX, 2), ("dp_0", "dp_1", "tp_0", "tp_1", "tp_2"))
    return jax.shard_map(
        per_device,
        mesh=finer,
        in_specs=(P(DP, TP, None), P(), P(DP, None, TP), P(DP, None, TP), P(None, TP), P(None, TP)),
        out_specs=(P(DP, TP, None), P()),
        check_vma=False,
    )
```
